512 devices in a mesh: ref: 16 (over x, y_lo, core), dom: 32 (over z, y_hi).
Axes of the slice: x: 4, y: 4 (y_hi: 2, y_lo: 2; y = y_hi * 2 + y_lo), z: 16, core: 2. Of those that a mesh axis runs over, the one named last changes fastest.
Arguments:
- particles: bfloat16 [8192, 7168], P(('ref', 'dom')), may hold values from -16 to 16
- offsets: int32 [8192], P(('ref', 'dom')), may hold values from 0 to 8, as said below
- references: bfloat16 [512, 7168], P('ref'), may hold values from -0.6 to 0.6
- noise_weight: float32 [3584], replicated, may hold values from 0.06 to 0.24
- ref_class: int32 [512], replicated, may hold values from 0 to 7
- ref_orient: int32 [512], replicated, may hold values from 0 to 63
- class_logprior: float32 [8], replicated, may hold values from -1 to 1
- orient_logprior: float32 [64], replicated, may hold values from -1 to 1
Outputs:
- log_post: float32 [8192, 9, 512], P(('ref', 'dom'))
- class_sums: float32 [8, 7168], P(None, ('ref', 'dom'))
The draws below stay inside these ranges and needn't reach their ends.
Inputs may be any that keep to these rules, and one draw needn't show every extreme that they name: `offsets`: index of the prior's centre: horizontal step (o mod 3) - 1 pixels, vertical step floor(o / 3) - 1 pixels.
All inputs are finite; a program needn't handle non-finite values.
Results may differ from the reference program's by a relative error of at most 0.0042.
Values may be sent and summed in bfloat16 or wider, within the bound.
A program may use at most 64 MiB of HBM per device.

```python
import math
import jax
import jax.numpy as jnp
from jax import lax

K = 3584
CLASSES = 8
ORIENT = 64
SHIFTS = 9
REFS = 512
NPART = 8192


def shared_draw(key):
    ref_key = jax.random.fold_in(key, 101)
    offset_key = jax.random.fold_in(key, 102)
    ref_values = 0.1 * jnp.clip(jax.random.normal(ref_key, (REFS, 2 * K), jnp.float32), -6.0, 6.0)
    offset_values = jax.random.randint(offset_key, (NPART,), 0, SHIFTS, dtype=jnp.int32)
    return (ref_values, offset_values)


def draw_references(key, part):
    ref_values, offset_values = shared_draw(key)
    return ref_values.astype(jnp.bfloat16)


def draw_offsets(key, part):
    ref_values, offset_values = shared_draw(key)
    return offset_values


def draw_particles(key, part):
    noise_key = jax.random.fold_in(key, 103)
    drawn = jnp.clip(jax.random.normal(noise_key, (NPART, 2 * K), jnp.float32), -6.0, 6.0)
    return drawn.astype(jnp.bfloat16)


def with_ends(result, own_key, least, top_value):
    longest = result.shape.index(max(result.shape))
    spots = []
    for shift in (0, 1):
        where = [jax.random.randint(jax.random.fold_in(own_key, axis), (), 0, length) for axis, length in enumerate(result.shape)]
        where[longest] = (where[longest] + shift) % result.shape[longest]
        spots.append(tuple(where))
    return result.at[spots[0]].set(least).at[spots[1]].set(top_value)


def setup_inputs(seed: int = 0) -> dict:
    key_of = jax.random.split(jax.random.key(seed), 9)
    return {
        "particles": draw_particles(jax.random.fold_in(key_of[8], 71), 0),
        "offsets": draw_offsets(jax.random.fold_in(key_of[8], 71), 0),
        "references": draw_references(jax.random.fold_in(key_of[8], 71), 0),
        "noise_weight": jnp.clip(jnp.exp(jax.random.uniform(key_of[3], (K,), jnp.float32, math.log(0.06), math.log(0.24))), 0.06, 0.24),
        "ref_class": with_ends(jax.random.randint(key_of[4], (REFS,), 0, CLASSES), jax.random.fold_in(key_of[4], 1), 0, CLASSES - 1).astype(jnp.int32),
        "ref_orient": with_ends(jax.random.randint(key_of[5], (REFS,), 0, ORIENT), jax.random.fold_in(key_of[5], 1), 0, ORIENT - 1).astype(jnp.int32),
        "class_logprior": jnp.clip(jax.random.uniform(key_of[6], (CLASSES,), jnp.float32, -1.0, 1.0), -1.0, 1.0),
        "orient_logprior": jnp.clip(jax.random.uniform(key_of[7], (ORIENT,), jnp.float32, -1.0, 1.0), -1.0, 1.0),
    }


def shift_tables(count):
    coeffs = jnp.arange(count, dtype=jnp.int32)
    column_freq = (coeffs % 56).astype(jnp.float32)
    row_freq = (coeffs // 56 - 32).astype(jnp.float32)
    shift_ids = jnp.arange(SHIFTS, dtype=jnp.int32)
    step_right = (shift_ids % 3 - 1).astype(jnp.float32)
    step_down = (shift_ids // 3 - 1).astype(jnp.float32)
    turning = 2.0 * math.pi / 96.0 * (step_right[:, None] * column_freq[None, :] + step_down[:, None] * row_freq[None, :])
    return (jnp.cos(turning), jnp.sin(turning))

def centre_prior(offsets):
    shift_ids = jnp.arange(SHIFTS, dtype=jnp.int32)
    step_right = (shift_ids % 3 - 1).astype(jnp.float32)
    step_down = (shift_ids // 3 - 1).astype(jnp.float32)
    centre_right = (offsets % 3 - 1).astype(jnp.float32)
    centre_down = (offsets // 3 - 1).astype(jnp.float32)
    apart_right = step_right[None, :] - centre_right[:, None]
    apart_down = step_down[None, :] - centre_down[:, None]
    return -0.5 * (apart_right * apart_right + apart_down * apart_down)

def aligned_stack(real_part, imag_part, cosine_table, sine_table, twice):
    turned_real = real_part[:, None, :] * cosine_table[None] - imag_part[:, None, :] * sine_table[None]
    turned_imag = real_part[:, None, :] * sine_table[None] + imag_part[:, None, :] * cosine_table[None]
    stacked_rows = real_part.shape[0] * cosine_table.shape[0]
    scaled_real = (turned_real * twice[None, None, :]).astype(jnp.bfloat16).reshape(stacked_rows, real_part.shape[1])
    scaled_imag = (turned_imag * twice[None, None, :]).astype(jnp.bfloat16).reshape(stacked_rows, real_part.shape[1])
    return (scaled_real, scaled_imag)

def reference(particles, offsets, references, noise_weight, ref_class, ref_orient, class_logprior, orient_logprior):
    cosine_table, sine_table = shift_tables(K)
    twice = 2.0 * noise_weight
    refs_wide = references.astype(jnp.float32)
    ref_norm = lax.optimization_barrier(jnp.sum(noise_weight[None, :] * (refs_wide[:, :K] * refs_wide[:, :K] + refs_wide[:, K:] * refs_wide[:, K:]), axis=1))
    class_table = (ref_class[:, None] == jnp.arange(CLASSES, dtype=jnp.int32)[None, :]).astype(jnp.float32)
    orient_table = (ref_orient[:, None] == jnp.arange(ORIENT, dtype=jnp.int32)[None, :]).astype(jnp.float32)
    prior = jnp.dot(class_table, class_logprior, precision=lax.Precision.HIGHEST) + jnp.dot(orient_table, orient_logprior, precision=lax.Precision.HIGHEST)
    block_rows = math.gcd(NPART, 1024)
    nblocks = NPART // block_rows
    stacked = particles.reshape(nblocks, block_rows, 2 * K)
    stacked_offsets = offsets.reshape(nblocks, block_rows)

    def visit(running, inputs):
        block, block_offsets = inputs
        values = block.astype(jnp.float32)
        real_part = values[:, :K]
        imag_part = values[:, K:]
        scaled_real, scaled_imag = aligned_stack(real_part, imag_part, cosine_table, sine_table, twice)
        cross = jnp.dot(scaled_real, references[:, :K].T, preferred_element_type=jnp.float32) + jnp.dot(scaled_imag, references[:, K:].T, preferred_element_type=jnp.float32)
        scores = cross.reshape(block_rows, SHIFTS, REFS) - ref_norm[None, None, :] + prior[None, None, :] + centre_prior(block_offsets)[:, :, None]
        row_peak = lax.optimization_barrier(jnp.max(scores, axis=(1, 2), keepdims=True))
        log_total = row_peak + jnp.log(lax.optimization_barrier(jnp.sum(jnp.exp(scores - row_peak), axis=(1, 2), keepdims=True)))
        log_post = scores - log_total
        class_post = jnp.dot(jnp.exp(log_post).reshape(block_rows * SHIFTS, REFS), class_table, precision=lax.Precision.HIGHEST).reshape(block_rows, SHIFTS, CLASSES)
        sums_real = jnp.einsum('ntc,nk->tck', class_post, real_part, precision=lax.Precision.HIGHEST)
        sums_imag = jnp.einsum('ntc,nk->tck', class_post, imag_part, precision=lax.Precision.HIGHEST)
        return ((running[0] + sums_real, running[1] + sums_imag), log_post)
    initial = (jnp.zeros((SHIFTS, CLASSES, K), jnp.float32), jnp.zeros((SHIFTS, CLASSES, K), jnp.float32))
    running, posts = lax.scan(visit, initial, (stacked, stacked_offsets))
    sums_real, sums_imag = running
    class_real = jnp.einsum('tk,tck->ck', cosine_table, sums_real, precision=lax.Precision.HIGHEST) - jnp.einsum('tk,tck->ck', sine_table, sums_imag, precision=lax.Precision.HIGHEST)
    class_imag = jnp.einsum('tk,tck->ck', sine_table, sums_real, precision=lax.Precision.HIGHEST) + jnp.einsum('tk,tck->ck', cosine_table, sums_imag, precision=lax.Precision.HIGHEST)
    class_sums = jnp.concatenate([class_real, class_imag], axis=1) * (1.0 / math.sqrt(NPART))
    return (posts.reshape(NPART, SHIFTS, REFS), class_sums)
```

```python
import functools
import math

import jax
import jax.numpy as jnp
import numpy as np
from jax import lax
from jax.experimental import pallas as pl
from jax.experimental.pallas import tpu as pltpu
from jax.sharding import PartitionSpec as P

MESH = pl.DeviceIdType.MESH
SHIFTS = 9
NX = 4
NS = 4
NZ = 16
NG = 8
NQ = 4
LANES = 128
F32 = jnp.float32
BF16 = jnp.bfloat16
PAIRS = ((5, 3), (7, 1), (8, 0), (6, 2))
STEPS = ((1, 0), (0, 1), (1, 1), (-1, 1))


def phase_tables(count):
    coeffs = np.arange(count)
    fx = (coeffs % 56).astype(np.float32)
    fy = (coeffs // 56 - 32).astype(np.float32)
    rows = []
    for sx, sy in STEPS:
        turning = np.float32(2.0 * math.pi / 96.0) * (np.float32(sx) * fx + np.float32(sy) * fy)
        turning = turning.astype(np.float64)
        rows += [np.cos(turning), np.sin(turning)]
    table = np.stack(rows).astype(np.float32)
    return np.ascontiguousarray(table.reshape(len(rows), -1, LANES).swapaxes(0, 1))


def nt(a, b):
    return lax.dot_general(a, b, (((1,), (1,)), ((), ())), preferred_element_type=F32)


def nn(a, b):
    return lax.dot_general(a, b, (((1,), (0,)), ((), ())), preferred_element_type=F32)


def split(value):
    high = value.astype(BF16)
    return high, (value - high.astype(F32)).astype(BF16)


def kernel(
    coefs,
    npart,
    rows,
    nref,
    classes,
    orients,
    off_hbm,
    clp_hbm,
    olp_hbm,
    part_hbm,
    refs_hbm,
    w_hbm,
    cls_hbm,
    ori_hbm,
    tab_hbm,
    post_out,
    sums_out,
    off,
    clp,
    olp,
    w,
    cls,
    ori,
    tab,
    tw,
    pb,
    rb,
    sp,
    s,
    na,
    spv,
    espb,
    gb,
    lz,
    sr,
    cb,
    wb,
    yb,
    tb,
    zb,
    far,
    sm,
    lp,
    lr,
    s_right,
    s_left,
    s_fwd,
    r_left,
    r_right,
    r_opp,
    s_y,
    s_p,
    s_py,
    r_y,
    r_p,
    r_py,
    s_e,
    r_e,
    s_g,
    r_g,
    s_s,
    r_s,
    s_w,
    r_w,
    s_z,
    r_z,
):
    ck = coefs // NQ
    me = lax.axis_index("ref")
    dm = lax.axis_index("dom")
    x = me // NS
    sub = me % NS
    yl = sub // 2
    core = sub % 2
    z = dm // 2
    yh = dm % 2
    group = sub * 2 + yh
    right = (me + NS) % (NX * NS)
    left = (me + (NX - 1) * NS) % (NX * NS)
    opposite = (me + 2 * NS) % (NX * NS)
    xl = (x + NX - 1) % NX
    xr = (x + 1) % NX
    partner = me + 1 - 2 * core
    y_ref = me + 2 - 4 * yl
    y_dom = dm + core * (1 - 2 * yh)
    refs = nref

    def remote(src, dst, send, recv, ref, dom):
        return pltpu.make_async_remote_copy(
            src_ref=src,
            dst_ref=dst,
            send_sem=send,
            recv_sem=recv,
            device_id=(ref, dom),
            device_id_type=MESH,
        )

    def arrived(buffer, sem):
        pltpu.make_async_copy(buffer, buffer, sem).wait()

    smalls = (
        (off_hbm, off),
        (clp_hbm, clp),
        (olp_hbm, olp),
        (w_hbm, w),
        (cls_hbm, cls),
        (ori_hbm, ori),
        (tab_hbm, tab),
    )
    own_rows = pl.ds(pl.multiple_of(sub * refs, refs), refs)
    for q in range(NQ):
        for half in range(2):
            pltpu.make_async_copy(
                part_hbm.at[:, pl.ds(half * coefs + q * ck, ck)],
                pb.at[x, q, :, pl.ds(half * ck, ck)],
                lp.at[q],
            ).start()
            pltpu.make_async_copy(
                refs_hbm.at[:, pl.ds(half * coefs + q * ck, ck)],
                rb.at[q, own_rows, pl.ds(half * ck, ck)],
                lr.at[q],
            ).start()
    for i, (src, dst) in enumerate(smalls):
        pltpu.make_async_copy(src, dst, sm.at[i]).start()

    barrier = pltpu.get_barrier_semaphore()

    def beside(distance, act):
        @pl.when(z >= distance)
        def _():
            act(me, dm - 2 * distance)

        @pl.when(z + distance < NZ)
        def _():
            act(me, dm + 2 * distance)

    def near(distance):
        return (z + NZ - distance) // NZ + (2 * NZ - 1 - z - distance) // NZ

    def greet(ref, dom):
        pl.semaphore_signal(barrier, inc=1, device_id=(ref, dom), device_id_type=MESH)

    for step in range(1, NX):
        greet((me + step * NS) % (NX * NS), dm)
    for step in range(1, NG):
        other = (group + step) % NG
        greet(x * NS + other // 2, z * 2 + other % 2)
    beside(1, greet)
    pl.semaphore_wait(barrier, NX - 1 + NG - 1 + near(1))

    def tell(i):
        def one(ref, dom):
            pl.semaphore_signal(far.at[i], inc=1, device_id=(ref, dom), device_id_type=MESH)

        beside(2**i, one)

    def heard(i):
        pl.semaphore_wait(far.at[i], near(2**i))

    tell(0)

    sends = []

    def go(copy):
        copy.start()
        sends.append(copy)

    def send_own(q):
        go(remote(pb.at[x, q], pb.at[x, q], s_right.at[q], r_left.at[q], right, dm))
        go(remote(pb.at[x, q], pb.at[x, q], s_left.at[q], r_right.at[q], left, dm))

    def forward(q):
        if q % 2 == 0:
            arrived(pb.at[xl, q], r_left.at[q])
            go(remote(pb.at[xl, q], pb.at[xl, q], s_fwd.at[q], r_opp.at[q], right, dm))
        else:
            arrived(pb.at[xr, q], r_right.at[q])
            go(remote(pb.at[xr, q], pb.at[xr, q], s_fwd.at[q], r_opp.at[q], left, dm))

    y_rows = pl.ds(pl.multiple_of((y_ref % NS) * refs, refs), refs)
    p_rows = pl.ds(pl.multiple_of((partner % NS) * refs, refs), refs)
    py_sub = (partner % NS) + 2 - 4 * yl
    py_rows = pl.ds(pl.multiple_of(py_sub * refs, refs), refs)

    for q in range(NQ):
        arrived(pb.at[x, q], lp.at[q])
        arrived(rb.at[q, own_rows], lr.at[q])
        if q < 2:
            send_own(q)
        own = rb.at[q, own_rows]
        go(remote(own, own, s_y.at[q], r_y.at[q], y_ref, y_dom))
        go(remote(own, own, s_p.at[q], r_p.at[q], partner, dm))

    for i, (src, dst) in enumerate(smalls):
        pltpu.make_async_copy(src, dst, sm.at[i]).wait()
    for i in range(coefs // LANES):
        two_w = 2.0 * w[i : i + 1, :]
        tw[i, 0:8, :] = tab[i] * two_w
        tw[i, 8:9, :] = two_w
    lane = lax.broadcasted_iota(jnp.int32, (1, LANES), 1)
    shift = lane // classes
    step_right = (shift % 3 - 1).astype(F32)
    step_down = (shift // 3 - 1).astype(F32)
    for n in range(rows):
        o = off[n]
        down = jnp.where(o >= 6, 2, jnp.where(o >= 3, 1, 0))
        centre_right = (o - 3 * down - 1).astype(F32)
        centre_down = (down - 1).astype(F32)
        apart_right = step_right - centre_right
        apart_down = step_down - centre_down
        spv[n : n + 1, :] = -0.5 * (apart_right * apart_right + apart_down * apart_down)
    used = lane < SHIFTS * classes
    espb[x] = jnp.where(used, jnp.exp(spv[...]), 0.0)
    for step, peer in enumerate((right, left, opposite)):
        go(remote(espb.at[x], espb.at[x], s_e.at[step], r_e.at[step], peer, dm))
    class_row = cls[pl.ds(x, 1), :]
    orient_row = ori[pl.ds(x, 1), :]
    prior = jnp.zeros((1, LANES), F32)
    for i in range(classes):
        prior = prior + jnp.where(class_row == i, clp[i], 0.0)
    orient_prior = jnp.zeros((1, LANES), F32)
    for i in range(orients):
        orient_prior = orient_prior + jnp.where(orient_row == i, olp[i], 0.0)
    prior = prior + orient_prior
    na[...] = jnp.zeros_like(na)
    s[...] = jnp.zeros_like(s)

    def compute(q):
        def tile(j, carry):
            at_real = pl.ds(pl.multiple_of(j * LANES, LANES), LANES)
            at_imag = pl.ds(pl.multiple_of(ck + j * LANES, LANES), LANES)
            at_table = q * (ck // LANES) + j
            real = pb[:, q, :, at_real].reshape(NX * rows, LANES).astype(F32)
            imag = pb[:, q, :, at_imag].reshape(NX * rows, LANES).astype(F32)

            def put(t, turned_real, turned_imag):
                sp[pl.ds(t * NX * rows, NX * rows), at_real] = turned_real.astype(BF16)
                sp[pl.ds(t * NX * rows, NX * rows), at_imag] = turned_imag.astype(BF16)

            plain = tw[at_table, 8:9, :]
            put(4, real * plain, imag * plain)
            for i, (plus, minus) in enumerate(PAIRS):
                cosine = tw[at_table, 2 * i : 2 * i + 1, :]
                sine = tw[at_table, 2 * i + 1 : 2 * i + 2, :]
                rc, rs = real * cosine, real * sine
                ic, is_ = imag * cosine, imag * sine
                put(plus, rc - is_, rs + ic)
                put(minus, rc + is_, ic - rs)
            weight = w[pl.ds(at_table, 1), :]
            ref_real = rb[q, :, at_real].astype(F32)
            ref_imag = rb[q, :, at_imag].astype(F32)
            na[...] += weight * (ref_real * ref_real + ref_imag * ref_imag)
            return carry

        lax.fori_loop(0, ck // LANES, tile, 0)
        s[...] += nt(sp[...], rb[q])

    def forward_refs(q):
        arrived(rb.at[q, y_rows], r_y.at[q])
        there = rb.at[q, y_rows]
        go(remote(there, there, s_py.at[q], r_py.at[q], partner, dm))

    def ready(q):
        if q % 2 == 0:
            arrived(pb.at[xr, q], r_right.at[q])
        else:
            arrived(pb.at[xl, q], r_left.at[q])
        arrived(pb.at[xl, q], r_opp.at[q])
        arrived(rb.at[q, p_rows], r_p.at[q])
        arrived(rb.at[q, py_rows], r_py.at[q])

    forward(0)
    send_own(2)
    forward_refs(0)
    forward(1)
    send_own(3)
    heard(0)
    tell(1)
    forward_refs(1)
    ready(0)
    compute(0)
    heard(1)
    tell(2)
    forward(2)
    forward_refs(2)
    ready(1)
    compute(1)
    forward(3)
    forward_refs(3)
    ready(2)
    compute(2)
    heard(2)
    tell(3)
    ready(3)
    compute(3)

    norm_row = jnp.sum(na[...].T, axis=0, keepdims=True)
    s[...] += prior - norm_row
    parts = NX * rows
    peak = s[0:parts, :]
    for t in range(1, SHIFTS):
        peak = jnp.maximum(peak, s[t * parts : (t + 1) * parts, :])
    peak = jnp.max(peak, axis=1, keepdims=True)
    column = lax.broadcasted_iota(jnp.int32, (LANES, LANES), 0)
    member = column % classes == class_row
    sums = jnp.zeros((parts, LANES), F32)
    for t in range(SHIFTS):
        chosen = jnp.where(member & (column // classes == t), 1.0, 0.0).astype(BF16)
        high, low = split(jnp.exp(s[t * parts : (t + 1) * parts, :] - peak))
        sums = sums + (nt(high, chosen) + nt(low, chosen))
    gb[x] = jnp.where(used, sums, peak)
    for step, peer in enumerate((right, left, opposite)):
        go(remote(gb.at[x], gb.at[x], s_g.at[step], r_g.at[step], peer, dm))
    s4 = s.reshape(SHIFTS, NX, rows, LANES)
    for step, peer in enumerate((right, left, opposite)):
        go(
            remote(
                s4.at[:, (x + (1, NX - 1, 2)[step]) % NX],
                sr.at[x],
                s_s.at[step],
                r_s.at[step],
                peer,
                dm,
            )
        )
    sr[x] = s4[:, x]

    for step in range(3):
        src = (x + (NX - 1, 1, 2)[step]) % NX
        arrived(espb.at[src], r_e.at[step])
    for step in range(3):
        src = (x + (NX - 1, 1, 2)[step]) % NX
        arrived(gb.at[src], r_g.at[step])
    peaks = [gb[i][:, LANES - 1 : LANES] for i in range(NX)]
    top = jnp.maximum(jnp.maximum(peaks[0], peaks[1]), jnp.maximum(peaks[2], peaks[3]))
    total = jnp.zeros((parts, LANES), F32)
    for i in range(NX):
        total = total + gb[i] * jnp.exp(peaks[i] - top)
    total = jnp.where(used, total, 0.0) * espb[...].reshape(parts, LANES)
    norm = jnp.sum(total, axis=1, keepdims=True)
    post = total * (1.0 / norm)
    lz[...] = jnp.broadcast_to(top + jnp.log(norm), (parts, LANES))

    turned = jnp.concatenate([post, jnp.zeros((LANES - parts, LANES), F32)], axis=0).T
    high, low = split(turned[: SHIFTS * classes, :parts])
    real_side = x < NX // 2
    at_e = pl.ds(pl.multiple_of(jnp.where(real_side, 0, ck), LANES), ck)
    at_f = pl.ds(pl.multiple_of(jnp.where(real_side, ck, 0), LANES), ck)
    sign = jnp.where(real_side, -1.0, 1.0).astype(F32) * (1.0 / math.sqrt(npart))
    scale = 1.0 / math.sqrt(npart)
    for piece in range(NQ // 2):
        q = (x % 2) * (NQ // 2) + piece
        e_rows = pb[:, q, :, at_e].reshape(parts, ck)
        f_rows = pb[:, q, :, at_f].reshape(parts, ck)
        e = nn(high, e_rows) + nn(low, e_rows)
        f = nn(high, f_rows) + nn(low, f_rows)
        for j in range(ck // LANES):
            at_table = q * (ck // LANES) + j

            def of(table, t):
                return table[t * classes : (t + 1) * classes, j * LANES : (j + 1) * LANES]

            even = of(e, 4)
            odd = jnp.zeros((classes, LANES), F32)
            for i, (plus, minus) in enumerate(PAIRS):
                cosine = tab[at_table, 2 * i : 2 * i + 1, :]
                sine = tab[at_table, 2 * i + 1 : 2 * i + 2, :]
                even = even + cosine * (of(e, plus) + of(e, minus))
                odd = odd + sine * (of(f, plus) - of(f, minus))
            at_column = piece * ck + j * LANES
            cb[:, at_column : at_column + LANES] = scale * even + sign * odd

    width = 2 * coefs // NX
    cols = width // LANES
    spread = LANES // classes
    k = lax.broadcasted_iota(jnp.int32, (spread, width), 1)
    keep = k % cols == lax.broadcasted_iota(jnp.int32, (spread, width), 0)
    d = lax.broadcasted_iota(jnp.int32, (LANES, width), 0)
    first = ((d // 32) * 32 + (d % 16) * 2 + (d // 16) % 2) * cols
    k = lax.broadcasted_iota(jnp.int32, (LANES, width), 1)
    pick = jnp.where((k >= first) & (k < first + cols), 1.0, 0.0).astype(BF16)
    laid = jnp.concatenate(
        [
            jnp.where(keep, jnp.broadcast_to(cb[i : i + 1, :], (spread, width)), 0.0)
            for i in [0, *range(classes - 1, 0, -1)]
        ],
        axis=0,
    )
    high, low = split(laid)
    wb[...] = (nt(pick, high) + nt(pick, low)).reshape(NG, NZ, LANES)
    for step in range(1, NG):
        other = (group + step) % NG
        go(
            remote(
                wb.at[other],
                yb.at[group],
                s_w.at[step],
                r_w.at[group],
                x * NS + other // 2,
                z * 2 + other % 2,
            )
        )
    yb[group] = wb[group]
    for step in range(1, NG):
        src = (group + step) % NG
        arrived(yb.at[src], r_w.at[src])
    heard(3)
    tb[...] = jnp.sum(yb[...], axis=0).reshape(NZ, 1, LANES)
    for step in range(1, NZ):
        other = (z + step) % NZ
        go(remote(tb.at[other], zb.at[z], s_z.at[step], r_z.at[z], me, other * 2 + yh))
    zb[z] = tb[z]

    for step in range(3):
        src = (x + (NX - 1, 1, 2)[step]) % NX
        arrived(sr.at[src], r_s.at[step])
    own_z = lz[pl.ds(pl.multiple_of(x * rows, rows), rows), :]
    for t in range(SHIFTS):
        bias = spv[:, t * classes : t * classes + 1] - own_z
        for i in range(NX):
            post_out[t, :, i * LANES : (i + 1) * LANES] = sr[i, t] + bias

    for step in range(1, NZ):
        src = (z + step) % NZ
        arrived(zb.at[src], r_z.at[src])
    final = jnp.sum(zb[...], axis=0)
    final = jnp.broadcast_to(final, (classes, LANES))
    final = pltpu.roll(final, 0, 1, stride=spread, stride_axis=0)
    sums_out[...] = final[:, :cols]
    for copy in sends:
        copy.wait_send()


def solution(mesh):
    assert mesh.shape["ref"] == NX * NS and mesh.shape["dom"] == 2 * NZ

    def local(particles, offsets, references, noise_weight, ref_class, ref_orient, class_logprior, orient_logprior):
        rows, both = particles.shape
        coefs = both // 2
        refs = references.shape[0]
        classes = class_logprior.shape[0]
        orients = orient_logprior.shape[0]
        ck = coefs // NQ
        parts = NX * rows
        width = both // NX
        cols = width // LANES
        npart = rows * NX * NS * 2 * NZ
        assert ck % LANES == 0 and refs * NS == LANES and SHIFTS * classes < LANES
        dma = pltpu.SemaphoreType.DMA
        log_post, class_sums = pl.pallas_call(
            functools.partial(kernel, coefs, npart, rows, refs, classes, orients),
            out_shape=(
                jax.ShapeDtypeStruct((SHIFTS, rows, NX * LANES), F32),
                jax.ShapeDtypeStruct((classes, cols), F32),
            ),
            in_specs=[pl.BlockSpec(memory_space=pltpu.HBM)] * 9,
            out_specs=(
                pl.BlockSpec(memory_space=pltpu.VMEM),
                pl.BlockSpec(memory_space=pltpu.VMEM),
            ),
            scratch_shapes=[
                pltpu.SMEM((rows,), jnp.int32),
                pltpu.SMEM((classes,), F32),
                pltpu.SMEM((orients,), F32),
                pltpu.VMEM((coefs // LANES, LANES), F32),
                pltpu.VMEM((NX, LANES), jnp.int32),
                pltpu.VMEM((NX, LANES), jnp.int32),
                pltpu.VMEM((coefs // LANES, 8, LANES), F32),
                pltpu.VMEM((coefs // LANES, 16, LANES), F32),
                pltpu.VMEM((NX, NQ, rows, 2 * ck), BF16),
                pltpu.VMEM((NQ, LANES, 2 * ck), BF16),
                pltpu.VMEM((SHIFTS * parts, 2 * ck), BF16),
                pltpu.VMEM((SHIFTS * parts, LANES), F32),
                pltpu.VMEM((LANES, LANES), F32),
                pltpu.VMEM((rows, LANES), F32),
                pltpu.VMEM((NX, rows, LANES), F32),
                pltpu.VMEM((NX, parts, LANES), F32),
                pltpu.VMEM((parts, LANES), F32),
                pltpu.VMEM((NX, SHIFTS, rows, LANES), F32),
                pltpu.VMEM((classes, width), F32),
                pltpu.VMEM((NG, NZ, LANES), F32),
                pltpu.VMEM((NG, NZ, LANES), F32),
                pltpu.VMEM((NZ, 1, LANES), F32),
                pltpu.VMEM((NZ, 1, LANES), F32),
                pltpu.SemaphoreType.REGULAR((4,)),
                dma((7,)),
            ]
            + [dma((NQ,))] * 14
            + [dma((3,))] * 6
            + [dma((NG,))] * 2
            + [dma((NZ,))] * 2,
            compiler_params=pltpu.CompilerParams(
                collective_id=0, has_side_effects=True, vmem_limit_bytes=67043328
            ),
            name="expectation",
        )(
            offsets,
            class_logprior,
            orient_logprior,
            particles,
            references,
            noise_weight.reshape(coefs // LANES, LANES),
            ref_class.reshape(NX, LANES),
            ref_orient.reshape(NX, LANES),
            jnp.asarray(phase_tables(coefs)),
        )
        return jnp.swapaxes(log_post, 0, 1), class_sums

    return jax.shard_map(
        local,
        mesh=mesh,
        in_specs=(
            P(("ref", "dom"), None),
            P(("ref", "dom")),
            P("ref", None),
            P(),
            P(),
            P(),
            P(),
            P(),
        ),
        out_specs=(P(("ref", "dom"), None, None), P(None, ("ref", "dom"))),
        check_vma=False,
    )
```

```python
import functools
import math

import jax
import jax.numpy as jnp
import numpy as np
from jax import lax
from jax.experimental import pallas as pl
from jax.experimental.pallas import tpu as pltpu
from jax.sharding import PartitionSpec as P

MESH = pl.DeviceIdType.MESH
SHIFTS = 9
NX = 4
NS = 4
NZ = 16
NG = 8
NQ = 7
AHEAD = 5
LANES = 128
F32 = jnp.float32
BF16 = jnp.bfloat16
PAIRS = ((5, 3), (7, 1), (8, 0), (6, 2))
STEPS = ((1, 0), (0, 1), (1, 1), (-1, 1))


def phase_tables(count):
    coeffs = np.arange(count)
    fx = (coeffs % 56).astype(np.float32)
    fy = (coeffs // 56 - 32).astype(np.float32)
    rows = []
    for sx, sy in STEPS:
        turning = np.float32(2.0 * math.pi / 96.0) * (np.float32(sx) * fx + np.float32(sy) * fy)
        turning = turning.astype(np.float64)
        rows += [np.cos(turning), np.sin(turning)]
    table = np.stack(rows).astype(np.float32)
    return np.ascontiguousarray(table.reshape(len(rows), -1, LANES).swapaxes(0, 1))


def nt(a, b):
    return lax.dot_general(a, b, (((1,), (1,)), ((), ())), preferred_element_type=F32)


def nn(a, b):
    return lax.dot_general(a, b, (((1,), (0,)), ((), ())), preferred_element_type=F32)


def split(value):
    high = value.astype(BF16)
    return high, (value - high.astype(F32)).astype(BF16)


def kernel(
    coefs,
    npart,
    rows,
    nref,
    classes,
    orients,
    off_hbm,
    clp_hbm,
    olp_hbm,
    part_hbm,
    refs_hbm,
    w_hbm,
    cls_hbm,
    ori_hbm,
    tab_hbm,
    post_out,
    sums_out,
    off,
    clp,
    olp,
    w,
    cls,
    ori,
    tab,
    tw,
    pb,
    rb,
    sp,
    s,
    na,
    spv,
    espb,
    gb,
    lz,
    chosen,
    keep,
    pick,
    sr,
    cb,
    wb,
    yb,
    tb,
    zb,
    far,
    sm,
    lp,
    lr,
    s_right,
    s_left,
    s_fwd,
    r_left,
    r_right,
    r_opp,
    s_y,
    s_p,
    s_py,
    r_y,
    r_p,
    r_py,
    s_e,
    r_e,
    s_g,
    r_g,
    s_s,
    r_s,
    s_w,
    r_w,
    s_z,
    r_z,
):
    ck = coefs // NQ
    me = lax.axis_index("ref")
    dm = lax.axis_index("dom")
    x = me // NS
    sub = me % NS
    yl = sub // 2
    core = sub % 2
    z = dm // 2
    yh = dm % 2
    group = sub * 2 + yh
    right = (me + NS) % (NX * NS)
    left = (me + (NX - 1) * NS) % (NX * NS)
    opposite = (me + 2 * NS) % (NX * NS)
    xl = (x + NX - 1) % NX
    xr = (x + 1) % NX
    partner = me + 1 - 2 * core
    y_ref = me + 2 - 4 * yl
    y_dom = dm + core * (1 - 2 * yh)
    refs = nref

    def remote(src, dst, send, recv, ref, dom):
        return pltpu.make_async_remote_copy(
            src_ref=src,
            dst_ref=dst,
            send_sem=send,
            recv_sem=recv,
            device_id=(ref, dom),
            device_id_type=MESH,
        )

    def arrived(buffer, sem):
        pltpu.make_async_copy(buffer, buffer, sem).wait()

    smalls = (
        (off_hbm, off),
        (clp_hbm, clp),
        (olp_hbm, olp),
        (w_hbm, w),
        (cls_hbm, cls),
        (ori_hbm, ori),
        (tab_hbm, tab),
    )
    own_rows = pl.ds(pl.multiple_of(sub * refs, refs), refs)
    for q in range(NQ):
        for half in range(2):
            pltpu.make_async_copy(
                part_hbm.at[:, pl.ds(half * coefs + q * ck, ck)],
                pb.at[x, q, :, pl.ds(half * ck, ck)],
                lp.at[q],
            ).start()
            pltpu.make_async_copy(
                refs_hbm.at[:, pl.ds(half * coefs + q * ck, ck)],
                rb.at[q, own_rows, pl.ds(half * ck, ck)],
                lr.at[q],
            ).start()
    for i, (src, dst) in enumerate(smalls):
        pltpu.make_async_copy(src, dst, sm.at[i]).start()

    barrier = pltpu.get_barrier_semaphore()

    def beside(distance, act):
        @pl.when(z >= distance)
        def _():
            act(me, dm - 2 * distance)

        @pl.when(z + distance < NZ)
        def _():
            act(me, dm + 2 * distance)

    def near(distance):
        return (z + NZ - distance) // NZ + (2 * NZ - 1 - z - distance) // NZ

    def greet(ref, dom):
        pl.semaphore_signal(barrier, inc=1, device_id=(ref, dom), device_id_type=MESH)

    for step in range(1, NX):
        greet((me + step * NS) % (NX * NS), dm)
    for step in range(1, NG):
        other = (group + step) % NG
        greet(x * NS + other // 2, z * 2 + other % 2)
    beside(1, greet)
    pl.semaphore_wait(barrier, NX - 1 + NG - 1 + near(1))

    def tell(i):
        def one(ref, dom):
            pl.semaphore_signal(far.at[i], inc=1, device_id=(ref, dom), device_id_type=MESH)

        beside(2**i, one)

    def heard(i):
        pl.semaphore_wait(far.at[i], near(2**i))

    tell(0)

    sends = []

    def go(copy):
        copy.start()
        sends.append(copy)

    def send_own(q):
        go(remote(pb.at[x, q], pb.at[x, q], s_right.at[q], r_left.at[q], right, dm))
        go(remote(pb.at[x, q], pb.at[x, q], s_left.at[q], r_right.at[q], left, dm))

    def forward(q):
        if q % 2 == 0:
            arrived(pb.at[xl, q], r_left.at[q])
            go(remote(pb.at[xl, q], pb.at[xl, q], s_fwd.at[q], r_opp.at[q], right, dm))
        else:
            arrived(pb.at[xr, q], r_right.at[q])
            go(remote(pb.at[xr, q], pb.at[xr, q], s_fwd.at[q], r_opp.at[q], left, dm))

    y_rows = pl.ds(pl.multiple_of((y_ref % NS) * refs, refs), refs)
    p_rows = pl.ds(pl.multiple_of((partner % NS) * refs, refs), refs)
    py_sub = (partner % NS) + 2 - 4 * yl
    py_rows = pl.ds(pl.multiple_of(py_sub * refs, refs), refs)

    for q in range(NQ):
        arrived(pb.at[x, q], lp.at[q])
        if q < AHEAD:
            send_own(q)
        arrived(rb.at[q, own_rows], lr.at[q])
        own = rb.at[q, own_rows]
        go(remote(own, own, s_y.at[q], r_y.at[q], y_ref, y_dom))
        go(remote(own, own, s_p.at[q], r_p.at[q], partner, dm))

    for i, (src, dst) in enumerate(smalls):
        pltpu.make_async_copy(src, dst, sm.at[i]).wait()
    for i in range(coefs // LANES):
        two_w = 2.0 * w[i : i + 1, :]
        tw[i, 0:8, :] = tab[i] * two_w
        tw[i, 8:9, :] = two_w
    lane = lax.broadcasted_iota(jnp.int32, (1, LANES), 1)
    shift = lane // classes
    step_right = (shift % 3 - 1).astype(F32)
    step_down = (shift // 3 - 1).astype(F32)
    for n in range(rows):
        o = off[n]
        down = jnp.where(o >= 6, 2, jnp.where(o >= 3, 1, 0))
        centre_right = (o - 3 * down - 1).astype(F32)
        centre_down = (down - 1).astype(F32)
        apart_right = step_right - centre_right
        apart_down = step_down - centre_down
        spv[n : n + 1, :] = -0.5 * (apart_right * apart_right + apart_down * apart_down)
    used = lane < SHIFTS * classes
    espb[x] = jnp.where(used, jnp.exp(spv[...]), 0.0)
    for step, peer in enumerate((right, left, opposite)):
        go(remote(espb.at[x], espb.at[x], s_e.at[step], r_e.at[step], peer, dm))
    class_row = cls[pl.ds(x, 1), :]
    orient_row = ori[pl.ds(x, 1), :]
    prior = jnp.zeros((1, LANES), F32)
    for i in range(classes):
        prior = prior + jnp.where(class_row == i, clp[i], 0.0)
    orient_prior = jnp.zeros((1, LANES), F32)
    for i in range(orients):
        orient_prior = orient_prior + jnp.where(orient_row == i, olp[i], 0.0)
    prior = prior + orient_prior
    column = lax.broadcasted_iota(jnp.int32, (LANES, LANES), 0)
    member = column % classes == class_row
    for t in range(SHIFTS):
        chosen[:, t * LANES : (t + 1) * LANES] = jnp.where(member & (column // classes == t), 1.0, 0.0).astype(BF16)
    width = 2 * coefs // NX
    cols = width // LANES
    spread = LANES // classes
    k = lax.broadcasted_iota(jnp.int32, (spread, width), 1)
    keep[...] = jnp.where(k % cols == lax.broadcasted_iota(jnp.int32, (spread, width), 0), 1.0, 0.0)
    d = lax.broadcasted_iota(jnp.int32, (LANES, width), 0)
    first = ((d // 32) * 32 + (d % 16) * 2 + (d // 16) % 2) * cols
    k = lax.broadcasted_iota(jnp.int32, (LANES, width), 1)
    pick[...] = jnp.where((k >= first) & (k < first + cols), 1.0, 0.0).astype(BF16)
    na[...] = jnp.zeros_like(na)
    s[...] = jnp.zeros_like(s)

    def compute(q):
        def tile(j, carry):
            at_real = pl.ds(pl.multiple_of(j * LANES, LANES), LANES)
            at_imag = pl.ds(pl.multiple_of(ck + j * LANES, LANES), LANES)
            at_table = q * (ck // LANES) + j
            real = pb[:, q, :, at_real].reshape(NX * rows, LANES).astype(F32)
            imag = pb[:, q, :, at_imag].reshape(NX * rows, LANES).astype(F32)

            def put(t, turned_real, turned_imag):
                sp[pl.ds(t * NX * rows, NX * rows), at_real] = turned_real.astype(BF16)
                sp[pl.ds(t * NX * rows, NX * rows), at_imag] = turned_imag.astype(BF16)

            plain = tw[at_table, 8:9, :]
            put(4, real * plain, imag * plain)
            for i, (plus, minus) in enumerate(PAIRS):
                cosine = tw[at_table, 2 * i : 2 * i + 1, :]
                sine = tw[at_table, 2 * i + 1 : 2 * i + 2, :]
                rc, rs = real * cosine, real * sine
                ic, is_ = imag * cosine, imag * sine
                put(plus, rc - is_, rs + ic)
                put(minus, rc + is_, ic - rs)
            weight = w[pl.ds(at_table, 1), :]
            ref_real = rb[q, :, at_real].astype(F32)
            ref_imag = rb[q, :, at_imag].astype(F32)
            na[...] += weight * (ref_real * ref_real + ref_imag * ref_imag)
            return carry

        lax.fori_loop(0, ck // LANES, tile, 0)
        s[...] += nt(sp[...], rb[q])

    def forward_refs(q):
        arrived(rb.at[q, y_rows], r_y.at[q])
        there = rb.at[q, y_rows]
        go(remote(there, there, s_py.at[q], r_py.at[q], partner, dm))

    def ready(q):
        if q % 2 == 0:
            arrived(pb.at[xr, q], r_right.at[q])
        else:
            arrived(pb.at[xl, q], r_left.at[q])
        arrived(pb.at[xl, q], r_opp.at[q])
        arrived(rb.at[q, p_rows], r_p.at[q])
        arrived(rb.at[q, py_rows], r_py.at[q])

    forward(0)
    send_own(AHEAD)
    forward_refs(0)
    heard(0)
    tell(1)
    forward(1)
    for q in range(AHEAD + 1, NQ):
        send_own(q)
    forward_refs(1)
    forward(2)
    forward(3)
    for q in range(NQ):
        if q + 2 < NQ:
            forward_refs(q + 2)
        ready(q)
        if q + 4 < NQ:
            forward(q + 4)
        compute(q)
        if q == 1:
            heard(1)
            tell(2)
        if q == 4:
            heard(2)
            tell(3)

    norm_row = jnp.sum(na[...].T, axis=0, keepdims=True)
    s[...] += prior - norm_row
    parts = NX * rows
    peak = s[0:parts, :]
    for t in range(1, SHIFTS):
        peak = jnp.maximum(peak, s[t * parts : (t + 1) * parts, :])
    peak = jnp.max(peak, axis=1, keepdims=True)
    peak_high, peak_low = split(peak)
    peak = peak_high.astype(F32) + peak_low.astype(F32)
    powers = [jnp.exp(s[t * parts : (t + 1) * parts, :] - peak).astype(BF16) for t in range(SHIFTS)]
    sums = nt(jnp.concatenate(powers, axis=1), chosen[...])
    tail = jnp.where(lane < LANES - 1, peak_high.astype(F32), peak_low.astype(F32))
    gb[x] = jnp.where(used, sums, tail).astype(BF16)
    for step, peer in enumerate((right, left, opposite)):
        go(remote(gb.at[x], gb.at[x], s_g.at[step], r_g.at[step], peer, dm))
    s4 = s.reshape(SHIFTS, NX, rows, LANES)
    for step, peer in enumerate((right, left, opposite)):
        go(
            remote(
                s4.at[:, (x + (1, NX - 1, 2)[step]) % NX],
                sr.at[x],
                s_s.at[step],
                r_s.at[step],
                peer,
                dm,
            )
        )
    sr[x] = s4[:, x]

    for step in range(3):
        src = (x + (NX - 1, 1, 2)[step]) % NX
        arrived(espb.at[src], r_e.at[step])
    for step in range(3):
        src = (x + (NX - 1, 1, 2)[step]) % NX
        arrived(gb.at[src], r_g.at[step])
    blocks = [gb[i].astype(F32) for i in range(NX)]
    peaks = [block[:, LANES - 2 : LANES - 1] + block[:, LANES - 1 : LANES] for block in blocks]
    top = jnp.maximum(jnp.maximum(peaks[0], peaks[1]), jnp.maximum(peaks[2], peaks[3]))
    total = jnp.zeros((parts, LANES), F32)
    for i in range(NX):
        total = total + blocks[i] * jnp.exp(peaks[i] - top)
    total = jnp.where(used, total, 0.0) * espb[...].reshape(parts, LANES)
    norm = jnp.sum(total, axis=1, keepdims=True)
    post = total * (1.0 / norm)
    lz[...] = jnp.broadcast_to(top + jnp.log(norm), (parts, LANES))

    turned = jnp.concatenate([post, jnp.zeros((LANES - parts, LANES), F32)], axis=0).T
    both = jnp.concatenate(split(turned[: SHIFTS * classes, :parts]), axis=0)
    pairs = SHIFTS * classes
    real_side = x < NX // 2
    sign = jnp.where(real_side, -1.0, 1.0).astype(F32) * (1.0 / math.sqrt(npart))
    scale = 1.0 / math.sqrt(npart)
    half = ck // 2
    for piece in range(NQ):
        place = (x % 2) * NQ + piece
        q = place // 2
        within = (place % 2) * half
        at_e = pl.ds(pl.multiple_of(within + jnp.where(real_side, 0, ck), LANES), half)
        at_f = pl.ds(pl.multiple_of(within + jnp.where(real_side, ck, 0), LANES), half)
        e = nn(both, pb[:, q, :, at_e].reshape(parts, half))
        f = nn(both, pb[:, q, :, at_f].reshape(parts, half))
        e = e[:pairs] + e[pairs:]
        f = f[:pairs] + f[pairs:]
        for j in range(half // LANES):
            at_table = place * (half // LANES) + j

            def of(table, t):
                return table[t * classes : (t + 1) * classes, j * LANES : (j + 1) * LANES]

            even = of(e, 4)
            odd = jnp.zeros((classes, LANES), F32)
            for i, (plus, minus) in enumerate(PAIRS):
                cosine = tab[at_table, 2 * i : 2 * i + 1, :]
                sine = tab[at_table, 2 * i + 1 : 2 * i + 2, :]
                even = even + cosine * (of(e, plus) + of(e, minus))
                odd = odd + sine * (of(f, plus) - of(f, minus))
            at_column = piece * half + j * LANES
            cb[:, at_column : at_column + LANES] = scale * even + sign * odd

    laid = jnp.concatenate(
        [
            (jnp.broadcast_to(cb[i : i + 1, :], (spread, width)) * keep[...]).astype(BF16)
            for i in [0, *range(classes - 1, 0, -1)]
        ],
        axis=0,
    )
    wb[...] = nt(pick[...], laid).reshape(NG, NZ, LANES).astype(BF16)
    for step in range(1, NG):
        other = (group + step) % NG
        go(
            remote(
                wb.at[other],
                yb.at[group],
                s_w.at[step],
                r_w.at[group],
                x * NS + other // 2,
                z * 2 + other % 2,
            )
        )
    yb[group] = wb[group]
    for step in range(1, NG):
        src = (group + step) % NG
        arrived(yb.at[src], r_w.at[src])
    heard(3)
    tb[...] = jnp.sum(yb[...].astype(F32), axis=0).reshape(NZ, 1, LANES)
    for step in range(1, NZ):
        other = (z + step) % NZ
        go(remote(tb.at[other], zb.at[z], s_z.at[step], r_z.at[z], me, other * 2 + yh))
    zb[z] = tb[z]

    for step in range(3):
        src = (x + (NX - 1, 1, 2)[step]) % NX
        arrived(sr.at[src], r_s.at[step])
    own_z = lz[pl.ds(pl.multiple_of(x * rows, rows), rows), :]
    for t in range(SHIFTS):
        bias = spv[:, t * classes : t * classes + 1] - own_z
        for i in range(NX):
            post_out[t, :, i * LANES : (i + 1) * LANES] = sr[i, t] + bias

    for step in range(1, NZ):
        src = (z + step) % NZ
        arrived(zb.at[src], r_z.at[src])
    final = jnp.sum(zb[...], axis=0)
    final = jnp.broadcast_to(final, (classes, LANES))
    final = pltpu.roll(final, 0, 1, stride=spread, stride_axis=0)
    sums_out[...] = final[:, :cols]
    for copy in sends:
        copy.wait_send()


def solution(mesh):
    assert mesh.shape["ref"] == NX * NS and mesh.shape["dom"] == 2 * NZ

    def local(particles, offsets, references, noise_weight, ref_class, ref_orient, class_logprior, orient_logprior):
        rows, both = particles.shape
        coefs = both // 2
        refs = references.shape[0]
        classes = class_logprior.shape[0]
        orients = orient_logprior.shape[0]
        ck = coefs // NQ
        parts = NX * rows
        width = both // NX
        cols = width // LANES
        npart = rows * NX * NS * 2 * NZ
        assert ck % LANES == 0 and refs * NS == LANES and SHIFTS * classes < LANES - 1 and ck % (2 * LANES) == 0
        dma = pltpu.SemaphoreType.DMA
        log_post, class_sums = pl.pallas_call(
            functools.partial(kernel, coefs, npart, rows, refs, classes, orients),
            out_shape=(
                jax.ShapeDtypeStruct((SHIFTS, rows, NX * LANES), F32),
                jax.ShapeDtypeStruct((classes, cols), F32),
            ),
            in_specs=[pl.BlockSpec(memory_space=pltpu.HBM)] * 9,
            out_specs=(
                pl.BlockSpec(memory_space=pltpu.VMEM),
                pl.BlockSpec(memory_space=pltpu.VMEM),
            ),
            scratch_shapes=[
                pltpu.SMEM((rows,), jnp.int32),
                pltpu.SMEM((classes,), F32),
                pltpu.SMEM((orients,), F32),
                pltpu.VMEM((coefs // LANES, LANES), F32),
                pltpu.VMEM((NX, LANES), jnp.int32),
                pltpu.VMEM((NX, LANES), jnp.int32),
                pltpu.VMEM((coefs // LANES, 8, LANES), F32),
                pltpu.VMEM((coefs // LANES, 16, LANES), F32),
                pltpu.VMEM((NX, NQ, rows, 2 * ck), BF16),
                pltpu.VMEM((NQ, LANES, 2 * ck), BF16),
                pltpu.VMEM((SHIFTS * parts, 2 * ck), BF16),
                pltpu.VMEM((SHIFTS * parts, LANES), F32),
                pltpu.VMEM((LANES, LANES), F32),
                pltpu.VMEM((rows, LANES), F32),
                pltpu.VMEM((NX, rows, LANES), F32),
                pltpu.VMEM((NX, parts, LANES), BF16),
                pltpu.VMEM((parts, LANES), F32),
                pltpu.VMEM((LANES, SHIFTS * LANES), BF16),
                pltpu.VMEM((LANES // classes, width), F32),
                pltpu.VMEM((LANES, width), BF16),
                pltpu.VMEM((NX, SHIFTS, rows, LANES), F32),
                pltpu.VMEM((classes, width), F32),
                pltpu.VMEM((NG, NZ, LANES), BF16),
                pltpu.VMEM((NG, NZ, LANES), BF16),
                pltpu.VMEM((NZ, 1, LANES), F32),
                pltpu.VMEM((NZ, 1, LANES), F32),
                pltpu.SemaphoreType.REGULAR((4,)),
                dma((7,)),
            ]
            + [dma((NQ,))] * 14
            + [dma((3,))] * 6
            + [dma((NG,))] * 2
            + [dma((NZ,))] * 2,
            compiler_params=pltpu.CompilerParams(
                collective_id=0, has_side_effects=True, vmem_limit_bytes=67043328
            ),
            name="expectation",
        )(
            offsets,
            class_logprior,
            orient_logprior,
            particles,
            references,
            noise_weight.reshape(coefs // LANES, LANES),
            ref_class.reshape(NX, LANES),
            ref_orient.reshape(NX, LANES),
            jnp.asarray(phase_tables(coefs)),
        )
        return jnp.swapaxes(log_post, 0, 1), class_sums

    return jax.shard_map(
        local,
        mesh=mesh,
        in_specs=(
            P(("ref", "dom"), None),
            P(("ref", "dom")),
            P("ref", None),
            P(),
            P(),
            P(),
            P(),
            P(),
        ),
        out_specs=(P(("ref", "dom"), None, None), P(None, ("ref", "dom"))),
        check_vma=False,
    )
```

```python
import functools
import math

import jax
import jax.numpy as jnp
import numpy as np
from jax import lax
from jax.experimental import pallas as pl
from jax.experimental.pallas import tpu as pltpu
from jax.sharding import PartitionSpec as P

MESH = pl.DeviceIdType.MESH
SHIFTS = 9
NX = 4
NS = 4
NZ = 16
NG = 8
NQ = 7
NEAR_LAG = 2
FAR_LAG = 4
AHEAD = 5
LANES = 128
F32 = jnp.float32
BF16 = jnp.bfloat16
PAIRS = ((5, 3), (7, 1), (8, 0), (6, 2))
STEPS = ((1, 0), (0, 1), (1, 1), (-1, 1))


def phase_tables(count):
    coeffs = np.arange(count)
    fx = (coeffs % 56).astype(np.float32)
    fy = (coeffs // 56 - 32).astype(np.float32)
    rows = []
    for sx, sy in STEPS:
        turning = np.float32(2.0 * math.pi / 96.0) * (np.float32(sx) * fx + np.float32(sy) * fy)
        turning = turning.astype(np.float64)
        rows += [np.cos(turning), np.sin(turning)]
    table = np.stack(rows).astype(np.float32)
    return np.ascontiguousarray(table.reshape(len(rows), -1, LANES).swapaxes(0, 1))


def nt(a, b):
    return lax.dot_general(a, b, (((1,), (1,)), ((), ())), preferred_element_type=F32)


def nn(a, b):
    return lax.dot_general(a, b, (((1,), (0,)), ((), ())), preferred_element_type=F32)


def split(value):
    high = value.astype(BF16)
    return high, (value - high.astype(F32)).astype(BF16)


def kernel(
    coefs,
    npart,
    rows,
    nref,
    classes,
    orients,
    off_hbm,
    clp_hbm,
    olp_hbm,
    part_hbm,
    refs_hbm,
    w_hbm,
    cls_hbm,
    ori_hbm,
    tab_hbm,
    post_out,
    sums_out,
    off,
    clp,
    olp,
    w,
    cls,
    ori,
    tab,
    tw,
    pb,
    rb,
    sp,
    sp_far,
    s,
    na,
    spv,
    espb,
    gb,
    lz,
    chosen,
    keep,
    pick,
    sr,
    cb,
    wb,
    yb,
    tb,
    zb,
    far,
    sm,
    lp,
    lr,
    s_right,
    s_left,
    s_fwd,
    r_left,
    r_right,
    r_opp,
    s_y,
    s_p,
    s_py,
    r_y,
    r_p,
    r_py,
    s_e,
    r_e,
    s_g,
    r_g,
    s_s,
    r_s,
    s_w,
    r_w,
    s_z,
    r_z,
):
    ck = coefs // NQ
    me = lax.axis_index("ref")
    dm = lax.axis_index("dom")
    x = me // NS
    sub = me % NS
    yl = sub // 2
    core = sub % 2
    z = dm // 2
    yh = dm % 2
    group = sub * 2 + yh
    right = (me + NS) % (NX * NS)
    left = (me + (NX - 1) * NS) % (NX * NS)
    opposite = (me + 2 * NS) % (NX * NS)
    xl = (x + NX - 1) % NX
    xr = (x + 1) % NX
    xo = (x + 2) % NX
    partner = me + 1 - 2 * core
    y_ref = me + 2 - 4 * yl
    y_dom = dm + core * (1 - 2 * yh)
    refs = nref

    def remote(src, dst, send, recv, ref, dom):
        return pltpu.make_async_remote_copy(
            src_ref=src,
            dst_ref=dst,
            send_sem=send,
            recv_sem=recv,
            device_id=(ref, dom),
            device_id_type=MESH,
        )

    def arrived(buffer, sem):
        pltpu.make_async_copy(buffer, buffer, sem).wait()

    smalls = (
        (off_hbm, off),
        (clp_hbm, clp),
        (olp_hbm, olp),
        (w_hbm, w),
        (cls_hbm, cls),
        (ori_hbm, ori),
        (tab_hbm, tab),
    )
    own_rows = pl.ds(pl.multiple_of(sub * refs, refs), refs)
    for q in range(NQ):
        for half in range(2):
            pltpu.make_async_copy(
                part_hbm.at[:, pl.ds(half * coefs + q * ck, ck)],
                pb.at[x, q, :, pl.ds(half * ck, ck)],
                lp.at[q],
            ).start()
            pltpu.make_async_copy(
                refs_hbm.at[:, pl.ds(half * coefs + q * ck, ck)],
                rb.at[q, own_rows, pl.ds(half * ck, ck)],
                lr.at[q],
            ).start()
    for i, (src, dst) in enumerate(smalls):
        pltpu.make_async_copy(src, dst, sm.at[i]).start()

    barrier = pltpu.get_barrier_semaphore()

    def beside(distance, act):
        @pl.when(z >= distance)
        def _():
            act(me, dm - 2 * distance)

        @pl.when(z + distance < NZ)
        def _():
            act(me, dm + 2 * distance)

    def near(distance):
        return (z + NZ - distance) // NZ + (2 * NZ - 1 - z - distance) // NZ

    def greet(ref, dom):
        pl.semaphore_signal(barrier, inc=1, device_id=(ref, dom), device_id_type=MESH)

    for step in range(1, NX):
        greet((me + step * NS) % (NX * NS), dm)
    for step in range(1, NG):
        other = (group + step) % NG
        greet(x * NS + other // 2, z * 2 + other % 2)
    beside(1, greet)
    pl.semaphore_wait(barrier, NX - 1 + NG - 1 + near(1))

    def tell(i):
        def one(ref, dom):
            pl.semaphore_signal(far.at[i], inc=1, device_id=(ref, dom), device_id_type=MESH)

        beside(2**i, one)

    def heard(i):
        pl.semaphore_wait(far.at[i], near(2**i))

    tell(0)

    sends = []

    def go(copy):
        copy.start()
        sends.append(copy)

    def send_own(q):
        go(remote(pb.at[x, q], pb.at[x, q], s_right.at[q], r_left.at[q], right, dm))
        go(remote(pb.at[x, q], pb.at[x, q], s_left.at[q], r_right.at[q], left, dm))

    def forward(q):
        if q % 2 == 0:
            arrived(pb.at[xl, q], r_left.at[q])
            go(remote(pb.at[xl, q], pb.at[xl, q], s_fwd.at[q], r_opp.at[q], right, dm))
        else:
            arrived(pb.at[xr, q], r_right.at[q])
            go(remote(pb.at[xr, q], pb.at[xr, q], s_fwd.at[q], r_opp.at[q], left, dm))

    y_rows = pl.ds(pl.multiple_of((y_ref % NS) * refs, refs), refs)
    p_rows = pl.ds(pl.multiple_of((partner % NS) * refs, refs), refs)
    py_sub = (partner % NS) + 2 - 4 * yl
    py_rows = pl.ds(pl.multiple_of(py_sub * refs, refs), refs)

    for q in range(NQ):
        arrived(pb.at[x, q], lp.at[q])
        if q < AHEAD:
            send_own(q)
        arrived(rb.at[q, own_rows], lr.at[q])
        own = rb.at[q, own_rows]
        go(remote(own, own, s_y.at[q], r_y.at[q], y_ref, y_dom))
        go(remote(own, own, s_p.at[q], r_p.at[q], partner, dm))

    for i, (src, dst) in enumerate(smalls):
        pltpu.make_async_copy(src, dst, sm.at[i]).wait()
    for i in range(coefs // LANES):
        two_w = 2.0 * w[i : i + 1, :]
        tw[i, 0:8, :] = tab[i] * two_w
        tw[i, 8:9, :] = two_w
    lane = lax.broadcasted_iota(jnp.int32, (1, LANES), 1)
    shift = lane // classes
    step_right = (shift % 3 - 1).astype(F32)
    step_down = (shift // 3 - 1).astype(F32)
    for n in range(rows):
        o = off[n]
        down = jnp.where(o >= 6, 2, jnp.where(o >= 3, 1, 0))
        centre_right = (o - 3 * down - 1).astype(F32)
        centre_down = (down - 1).astype(F32)
        apart_right = step_right - centre_right
        apart_down = step_down - centre_down
        spv[n : n + 1, :] = -0.5 * (apart_right * apart_right + apart_down * apart_down)
    used = lane < SHIFTS * classes
    espb[x] = jnp.where(used, jnp.exp(spv[...]), 0.0)
    for step, peer in enumerate((right, left, opposite)):
        go(remote(espb.at[x], espb.at[x], s_e.at[step], r_e.at[step], peer, dm))
    class_row = cls[pl.ds(x, 1), :]
    orient_row = ori[pl.ds(x, 1), :]
    prior = jnp.zeros((1, LANES), F32)
    for i in range(classes):
        prior = prior + jnp.where(class_row == i, clp[i], 0.0)
    orient_prior = jnp.zeros((1, LANES), F32)
    for i in range(orients):
        orient_prior = orient_prior + jnp.where(orient_row == i, olp[i], 0.0)
    prior = prior + orient_prior
    column = lax.broadcasted_iota(jnp.int32, (LANES, LANES), 0)
    member = column % classes == class_row
    for t in range(SHIFTS):
        chosen[:, t * LANES : (t + 1) * LANES] = jnp.where(member & (column // classes == t), 1.0, 0.0).astype(BF16)
    width = 2 * coefs // NX
    cols = width // LANES
    spread = LANES // classes
    k = lax.broadcasted_iota(jnp.int32, (spread, width), 1)
    keep[...] = jnp.where(k % cols == lax.broadcasted_iota(jnp.int32, (spread, width), 0), 1.0, 0.0)
    d = lax.broadcasted_iota(jnp.int32, (LANES, width), 0)
    first = ((d // 32) * 32 + (d % 16) * 2 + (d // 16) % 2) * cols
    k = lax.broadcasted_iota(jnp.int32, (LANES, width), 1)
    pick[...] = jnp.where((k >= first) & (k < first + cols), 1.0, 0.0).astype(BF16)
    na[...] = jnp.zeros_like(na)
    s[...] = jnp.zeros_like(s)

    block = SHIFTS * rows

    def turn(to, slot, xs, q):
        def tile(j, carry):
            at_real = pl.ds(pl.multiple_of(j * LANES, LANES), LANES)
            at_imag = pl.ds(pl.multiple_of(ck + j * LANES, LANES), LANES)
            at_table = q * (ck // LANES) + j
            real = pb[xs, q, :, at_real].astype(F32)
            imag = pb[xs, q, :, at_imag].astype(F32)

            def put(t, turned_real, turned_imag):
                at_rows = pl.ds(slot * block + t * rows, rows)
                to[at_rows, at_real] = turned_real.astype(BF16)
                to[at_rows, at_imag] = turned_imag.astype(BF16)

            plain = tw[at_table, 8:9, :]
            put(4, real * plain, imag * plain)
            for i, (plus, minus) in enumerate(PAIRS):
                cosine = tw[at_table, 2 * i : 2 * i + 1, :]
                sine = tw[at_table, 2 * i + 1 : 2 * i + 2, :]
                rc, rs = real * cosine, real * sine
                ic, is_ = imag * cosine, imag * sine
                put(plus, rc - is_, rs + ic)
                put(minus, rc + is_, ic - rs)
            return carry

        for j in range(ck // LANES):
            tile(j, 0)

    def measure(q):
        def tile(j, carry):
            at_real = pl.ds(pl.multiple_of(j * LANES, LANES), LANES)
            at_imag = pl.ds(pl.multiple_of(ck + j * LANES, LANES), LANES)
            weight = w[pl.ds(q * (ck // LANES) + j, 1), :]
            ref_real = rb[q, :, at_real].astype(F32)
            ref_imag = rb[q, :, at_imag].astype(F32)
            na[...] += weight * (ref_real * ref_real + ref_imag * ref_imag)
            return carry

        lax.fori_loop(0, ck // LANES, tile, 0)

    near_rows = 3 * block

    def score_near(q):
        s[0:near_rows, :] += nt(sp[q], rb[q])

    def score_far(q):
        arrived(pb.at[xo, q], r_opp.at[q])
        turn(sp_far, 0, xo, q)
        s[near_rows:, :] += nt(sp_far[...], rb[q])

    def forward_refs(q):
        arrived(rb.at[q, y_rows], r_y.at[q])
        there = rb.at[q, y_rows]
        go(remote(there, there, s_py.at[q], r_py.at[q], partner, dm))

    def other_side(q):
        if q % 2 == 0:
            arrived(pb.at[xr, q], r_right.at[q])
        else:
            arrived(pb.at[xl, q], r_left.at[q])

    for q in range(NQ):
        turn(sp.at[q], 0, x, q)
    for q in range(NQ + FAR_LAG):
        if q < NQ:
            forward(q)
            if q == 0:
                send_own(AHEAD)
            if q == 1:
                for later in range(AHEAD + 1, NQ):
                    send_own(later)
            forward_refs(q)
            other_side(q)
            turn(sp.at[q], 1, xl, q)
            turn(sp.at[q], 2, xr, q)
        if 0 <= q - NEAR_LAG < NQ:
            arrived(rb.at[q - NEAR_LAG, p_rows], r_p.at[q - NEAR_LAG])
            arrived(rb.at[q - NEAR_LAG, py_rows], r_py.at[q - NEAR_LAG])
            score_near(q - NEAR_LAG)
            measure(q - NEAR_LAG)
        if q >= FAR_LAG:
            score_far(q - FAR_LAG)
        if q == 1:
            heard(0)
            tell(1)
        if q == 4:
            heard(1)
            tell(2)
    heard(2)
    tell(3)

    norm_row = jnp.sum(na[...].T, axis=0, keepdims=True)
    s[...] += prior - norm_row
    parts = NX * rows
    s4 = s.reshape(NX, SHIFTS, rows, LANES)
    by_shift = [s4[:, t].reshape(parts, LANES) for t in range(SHIFTS)]
    peak = functools.reduce(jnp.maximum, by_shift)
    peak = jnp.max(peak, axis=1, keepdims=True)
    peak_high, peak_low = split(peak)
    peak = peak_high.astype(F32) + peak_low.astype(F32)
    powers = [jnp.exp(value - peak).astype(BF16) for value in by_shift]
    sums = nt(jnp.concatenate(powers, axis=1), chosen[...])
    tail = jnp.where(lane < LANES - 1, peak_high.astype(F32), peak_low.astype(F32))
    packed = jnp.where(used, sums, tail).astype(BF16)
    for slot, xs in enumerate((x, xl, xr, xo)):
        gb[x, pl.ds(pl.multiple_of(xs * rows, rows), rows), :] = packed[slot * rows : (slot + 1) * rows]
    for step, peer in enumerate((right, left, opposite)):
        go(remote(gb.at[x], gb.at[x], s_g.at[step], r_g.at[step], peer, dm))
    for step, (slot, peer) in enumerate(((2, right), (1, left), (3, opposite))):
        go(remote(s4.at[slot], sr.at[x], s_s.at[step], r_s.at[step], peer, dm))
    sr[x] = s4[0]

    for step in range(3):
        src = (x + (NX - 1, 1, 2)[step]) % NX
        arrived(espb.at[src], r_e.at[step])
    for step in range(3):
        src = (x + (NX - 1, 1, 2)[step]) % NX
        arrived(gb.at[src], r_g.at[step])
    blocks = [gb[i].astype(F32) for i in range(NX)]
    peaks = [block[:, LANES - 2 : LANES - 1] + block[:, LANES - 1 : LANES] for block in blocks]
    top = jnp.maximum(jnp.maximum(peaks[0], peaks[1]), jnp.maximum(peaks[2], peaks[3]))
    total = jnp.zeros((parts, LANES), F32)
    for i in range(NX):
        total = total + blocks[i] * jnp.exp(peaks[i] - top)
    total = jnp.where(used, total, 0.0) * espb[...].reshape(parts, LANES)
    norm = jnp.sum(total, axis=1, keepdims=True)
    post = total * (1.0 / norm)
    lz[...] = jnp.broadcast_to(top + jnp.log(norm), (parts, LANES))

    turned = jnp.concatenate([post, jnp.zeros((LANES - parts, LANES), F32)], axis=0).T
    both = jnp.concatenate(split(turned[: SHIFTS * classes, :parts]), axis=0)
    pairs = SHIFTS * classes
    real_side = x < NX // 2
    sign = jnp.where(real_side, -1.0, 1.0).astype(F32) * (1.0 / math.sqrt(npart))
    scale = 1.0 / math.sqrt(npart)
    half = ck // 2
    for piece in range(NQ):
        place = (x % 2) * NQ + piece
        q = place // 2
        within = (place % 2) * half
        at_e = pl.ds(pl.multiple_of(within + jnp.where(real_side, 0, ck), LANES), half)
        at_f = pl.ds(pl.multiple_of(within + jnp.where(real_side, ck, 0), LANES), half)
        e = nn(both, pb[:, q, :, at_e].reshape(parts, half))
        f = nn(both, pb[:, q, :, at_f].reshape(parts, half))
        e = e[:pairs] + e[pairs:]
        f = f[:pairs] + f[pairs:]
        for j in range(half // LANES):
            at_table = place * (half // LANES) + j

            def of(table, t):
                return table[t * classes : (t + 1) * classes, j * LANES : (j + 1) * LANES]

            even = of(e, 4)
            odd = jnp.zeros((classes, LANES), F32)
            for i, (plus, minus) in enumerate(PAIRS):
                cosine = tab[at_table, 2 * i : 2 * i + 1, :]
                sine = tab[at_table, 2 * i + 1 : 2 * i + 2, :]
                even = even + cosine * (of(e, plus) + of(e, minus))
                odd = odd + sine * (of(f, plus) - of(f, minus))
            at_column = piece * half + j * LANES
            cb[:, at_column : at_column + LANES] = scale * even + sign * odd

    laid = jnp.concatenate(
        [
            (jnp.broadcast_to(cb[i : i + 1, :], (spread, width)) * keep[...]).astype(BF16)
            for i in [0, *range(classes - 1, 0, -1)]
        ],
        axis=0,
    )
    wb[...] = nt(pick[...], laid).reshape(NG, NZ, LANES).astype(BF16)
    for step in range(1, NG):
        other = (group + step) % NG
        go(
            remote(
                wb.at[other],
                yb.at[group],
                s_w.at[step],
                r_w.at[group],
                x * NS + other // 2,
                z * 2 + other % 2,
            )
        )
    yb[group] = wb[group]
    for step in range(1, NG):
        src = (group + step) % NG
        arrived(yb.at[src], r_w.at[src])
    heard(3)
    tb[...] = jnp.sum(yb[...].astype(F32), axis=0).reshape(NZ, 1, LANES)
    for step in range(1, NZ):
        other = (z + step) % NZ
        go(remote(tb.at[other], zb.at[z], s_z.at[step], r_z.at[z], me, other * 2 + yh))
    zb[z] = tb[z]

    for step in range(3):
        src = (x + (NX - 1, 1, 2)[step]) % NX
        arrived(sr.at[src], r_s.at[step])
    own_z = lz[pl.ds(pl.multiple_of(x * rows, rows), rows), :]
    for t in range(SHIFTS):
        bias = spv[:, t * classes : t * classes + 1] - own_z
        for i in range(NX):
            post_out[t, :, i * LANES : (i + 1) * LANES] = sr[i, t] + bias

    for step in range(1, NZ):
        src = (z + step) % NZ
        arrived(zb.at[src], r_z.at[src])
    final = jnp.sum(zb[...], axis=0)
    final = jnp.broadcast_to(final, (classes, LANES))
    final = pltpu.roll(final, 0, 1, stride=spread, stride_axis=0)
    sums_out[...] = final[:, :cols]
    for copy in sends:
        copy.wait_send()


def solution(mesh):
    assert mesh.shape["ref"] == NX * NS and mesh.shape["dom"] == 2 * NZ

    def local(particles, offsets, references, noise_weight, ref_class, ref_orient, class_logprior, orient_logprior):
        rows, both = particles.shape
        coefs = both // 2
        refs = references.shape[0]
        classes = class_logprior.shape[0]
        orients = orient_logprior.shape[0]
        ck = coefs // NQ
        parts = NX * rows
        width = both // NX
        cols = width // LANES
        npart = rows * NX * NS * 2 * NZ
        assert ck % LANES == 0 and refs * NS == LANES and SHIFTS * classes < LANES - 1 and ck % (2 * LANES) == 0
        dma = pltpu.SemaphoreType.DMA

        def hbm(array):
            return pltpu.with_memory_space_constraint(array, pltpu.HBM)

        log_post, class_sums = pl.pallas_call(
            functools.partial(kernel, coefs, npart, rows, refs, classes, orients),
            out_shape=(
                jax.ShapeDtypeStruct((SHIFTS, rows, NX * LANES), F32),
                jax.ShapeDtypeStruct((classes, cols), F32),
            ),
            in_specs=[pl.BlockSpec(memory_space=pltpu.HBM)] * 9,
            out_specs=(
                pl.BlockSpec(memory_space=pltpu.VMEM),
                pl.BlockSpec(memory_space=pltpu.VMEM),
            ),
            scratch_shapes=[
                pltpu.SMEM((rows,), jnp.int32),
                pltpu.SMEM((classes,), F32),
                pltpu.SMEM((orients,), F32),
                pltpu.VMEM((coefs // LANES, LANES), F32),
                pltpu.VMEM((NX, LANES), jnp.int32),
                pltpu.VMEM((NX, LANES), jnp.int32),
                pltpu.VMEM((coefs // LANES, 8, LANES), F32),
                pltpu.VMEM((coefs // LANES, 16, LANES), F32),
                pltpu.VMEM((NX, NQ, rows, 2 * ck), BF16),
                pltpu.VMEM((NQ, LANES, 2 * ck), BF16),
                pltpu.VMEM((NQ, SHIFTS * 3 * rows, 2 * ck), BF16),
                pltpu.VMEM((SHIFTS * rows, 2 * ck), BF16),
                pltpu.VMEM((SHIFTS * parts, LANES), F32),
                pltpu.VMEM((LANES, LANES), F32),
                pltpu.VMEM((rows, LANES), F32),
                pltpu.VMEM((NX, rows, LANES), F32),
                pltpu.VMEM((NX, parts, LANES), BF16),
                pltpu.VMEM((parts, LANES), F32),
                pltpu.VMEM((LANES, SHIFTS * LANES), BF16),
                pltpu.VMEM((LANES // classes, width), F32),
                pltpu.VMEM((LANES, width), BF16),
                pltpu.VMEM((NX, SHIFTS, rows, LANES), F32),
                pltpu.VMEM((classes, width), F32),
                pltpu.VMEM((NG, NZ, LANES), BF16),
                pltpu.VMEM((NG, NZ, LANES), BF16),
                pltpu.VMEM((NZ, 1, LANES), F32),
                pltpu.VMEM((NZ, 1, LANES), F32),
                pltpu.SemaphoreType.REGULAR((4,)),
                dma((7,)),
            ]
            + [dma((NQ,))] * 14
            + [dma((3,))] * 6
            + [dma((NG,))] * 2
            + [dma((NZ,))] * 2,
            compiler_params=pltpu.CompilerParams(
                collective_id=0, has_side_effects=True, vmem_limit_bytes=32 * 1024 * 1024
            ),
            name="expectation",
        )(
            hbm(offsets),
            hbm(class_logprior),
            hbm(orient_logprior),
            hbm(particles),
            hbm(references),
            hbm(noise_weight.reshape(coefs // LANES, LANES)),
            hbm(ref_class.reshape(NX, LANES)),
            hbm(ref_orient.reshape(NX, LANES)),
            hbm(jnp.asarray(phase_tables(coefs))),
        )
        return jnp.swapaxes(log_post, 0, 1), class_sums

    return jax.shard_map(
        local,
        mesh=mesh,
        in_specs=(
            P(("ref", "dom"), None),
            P(("ref", "dom")),
            P("ref", None),
            P(),
            P(),
            P(),
            P(),
            P(),
        ),
        out_specs=(P(("ref", "dom"), None, None), P(None, ("ref", "dom"))),
        check_vma=False,
    )
```

```python
import functools
import math

import jax
import jax.numpy as jnp
import numpy as np
from jax import lax
from jax.experimental import pallas as pl
from jax.experimental.pallas import tpu as pltpu
from jax.sharding import PartitionSpec as P

MESH = pl.DeviceIdType.MESH
SHIFTS = 9
NX = 4
NS = 4
NZ = 16
NG = 8
NQ = 7
NEAR_LAG = 1
HELD = 2
LANES = 128
F32 = jnp.float32
BF16 = jnp.bfloat16
PAIRS = ((5, 3), (7, 1), (8, 0), (6, 2))
STEPS = ((1, 0), (0, 1), (1, 1), (-1, 1))


def phase_tables(count):
    coeffs = np.arange(count)
    fx = (coeffs % 56).astype(np.float32)
    fy = (coeffs // 56 - 32).astype(np.float32)
    rows = []
    for sx, sy in STEPS:
        turning = np.float32(2.0 * math.pi / 96.0) * (np.float32(sx) * fx + np.float32(sy) * fy)
        turning = turning.astype(np.float64)
        rows += [np.cos(turning), np.sin(turning)]
    table = np.stack(rows).astype(np.float32)
    return np.ascontiguousarray(table.reshape(len(rows), -1, LANES).swapaxes(0, 1))


def nt(a, b):
    return lax.dot_general(a, b, (((1,), (1,)), ((), ())), preferred_element_type=F32)


def nn(a, b):
    return lax.dot_general(a, b, (((1,), (0,)), ((), ())), preferred_element_type=F32)


def split(value):
    high = value.astype(BF16)
    return high, (value - high.astype(F32)).astype(BF16)


def kernel(
    coefs,
    npart,
    rows,
    nref,
    classes,
    orients,
    off_hbm,
    clp_hbm,
    olp_hbm,
    part_hbm,
    refs_hbm,
    w_hbm,
    cls_hbm,
    ori_hbm,
    tab_hbm,
    post_out,
    sums_out,
    off,
    clp,
    olp,
    w,
    cls,
    ori,
    tab,
    tw,
    pb,
    rb,
    sp,
    sp_far,
    s,
    na,
    spv,
    espb,
    gb,
    lz,
    chosen,
    keep,
    pick,
    sr,
    cb,
    wb,
    yb,
    tb,
    zb,
    far,
    sm,
    lp,
    lr,
    s_right,
    s_left,
    s_fwd,
    r_left,
    r_right,
    r_opp,
    s_y,
    s_p,
    s_py,
    r_y,
    r_p,
    r_py,
    s_e,
    r_e,
    s_g,
    r_g,
    s_s,
    r_s,
    s_w,
    r_w,
    s_z,
    r_z,
):
    ck = coefs // NQ
    me = lax.axis_index("ref")
    dm = lax.axis_index("dom")
    x = me // NS
    sub = me % NS
    yl = sub // 2
    core = sub % 2
    z = dm // 2
    yh = dm % 2
    group = sub * 2 + yh
    right = (me + NS) % (NX * NS)
    left = (me + (NX - 1) * NS) % (NX * NS)
    opposite = (me + 2 * NS) % (NX * NS)
    xl = (x + NX - 1) % NX
    xr = (x + 1) % NX
    xo = (x + 2) % NX
    partner = me + 1 - 2 * core
    y_ref = me + 2 - 4 * yl
    y_dom = dm + core * (1 - 2 * yh)
    refs = nref

    def remote(src, dst, send, recv, ref, dom):
        return pltpu.make_async_remote_copy(
            src_ref=src,
            dst_ref=dst,
            send_sem=send,
            recv_sem=recv,
            device_id=(ref, dom),
            device_id_type=MESH,
        )

    def arrived(buffer, sem):
        pltpu.make_async_copy(buffer, buffer, sem).wait()

    smalls = (
        (off_hbm, off),
        (clp_hbm, clp),
        (olp_hbm, olp),
        (w_hbm, w),
        (cls_hbm, cls),
        (ori_hbm, ori),
        (tab_hbm, tab),
    )
    own_rows = pl.ds(pl.multiple_of(sub * refs, refs), refs)
    for q in range(NQ):
        for half in range(2):
            pltpu.make_async_copy(
                part_hbm.at[:, pl.ds(half * coefs + q * ck, ck)],
                pb.at[x, q, :, pl.ds(half * ck, ck)],
                lp.at[q],
            ).start()
            pltpu.make_async_copy(
                refs_hbm.at[:, pl.ds(half * coefs + q * ck, ck)],
                rb.at[q, own_rows, pl.ds(half * ck, ck)],
                lr.at[q],
            ).start()
    for i, (src, dst) in enumerate(smalls):
        pltpu.make_async_copy(src, dst, sm.at[i]).start()

    barrier = pltpu.get_barrier_semaphore()

    def beside(distance, act):
        @pl.when(z >= distance)
        def _():
            act(me, dm - 2 * distance)

        @pl.when(z + distance < NZ)
        def _():
            act(me, dm + 2 * distance)

    def near(distance):
        return (z + NZ - distance) // NZ + (2 * NZ - 1 - z - distance) // NZ

    def greet(ref, dom):
        pl.semaphore_signal(barrier, inc=1, device_id=(ref, dom), device_id_type=MESH)

    for step in range(1, NX):
        greet((me + step * NS) % (NX * NS), dm)
    for step in range(1, NG):
        other = (group + step) % NG
        greet(x * NS + other // 2, z * 2 + other % 2)
    beside(1, greet)
    pl.semaphore_wait(barrier, NX - 1 + NG - 1 + near(1))

    def tell(i):
        def one(ref, dom):
            pl.semaphore_signal(far.at[i], inc=1, device_id=(ref, dom), device_id_type=MESH)

        beside(2**i, one)

    def heard(i):
        pl.semaphore_wait(far.at[i], near(2**i))

    tell(0)

    sends = []

    def go(copy):
        copy.start()
        sends.append(copy)

    def send_own(q):
        go(remote(pb.at[x, q], pb.at[x, q], s_right.at[q], r_left.at[q], right, dm))
        go(remote(pb.at[x, q], pb.at[x, q], s_left.at[q], r_right.at[q], left, dm))

    def forward(q):
        if q % 2 == 0:
            arrived(pb.at[xl, q], r_left.at[q])
        if q % 2 == 1 or q == NQ - 1:
            arrived(pb.at[xr, q], r_right.at[q])
        if q == NQ - 1:
            for way, (xs, peer) in enumerate(((xl, right), (xr, left))):
                piece = pb.at[xs, q, :, way * ck : (way + 1) * ck]
                go(remote(piece, piece, s_fwd.at[q + way], r_opp.at[q + way], peer, dm))
        elif q % 2 == 0:
            go(remote(pb.at[xl, q], pb.at[xl, q], s_fwd.at[q], r_opp.at[q], right, dm))
        else:
            go(remote(pb.at[xr, q], pb.at[xr, q], s_fwd.at[q], r_opp.at[q], left, dm))

    y_rows = pl.ds(pl.multiple_of((y_ref % NS) * refs, refs), refs)
    p_rows = pl.ds(pl.multiple_of((partner % NS) * refs, refs), refs)
    py_sub = (partner % NS) + 2 - 4 * yl
    py_rows = pl.ds(pl.multiple_of(py_sub * refs, refs), refs)

    for q in range(NQ):
        arrived(pb.at[x, q], lp.at[q])
        send_own(q)
        arrived(rb.at[q, own_rows], lr.at[q])
        own = rb.at[q, own_rows]
        go(remote(own, own, s_y.at[q], r_y.at[q], y_ref, y_dom))
        go(remote(own, own, s_p.at[q], r_p.at[q], partner, dm))

    for i, (src, dst) in enumerate(smalls):
        pltpu.make_async_copy(src, dst, sm.at[i]).wait()
    for i in range(coefs // LANES):
        two_w = 2.0 * w[i : i + 1, :]
        tw[i, 0:8, :] = tab[i] * two_w
        tw[i, 8:9, :] = two_w
    lane = lax.broadcasted_iota(jnp.int32, (1, LANES), 1)
    shift = lane // classes
    step_right = (shift % 3 - 1).astype(F32)
    step_down = (shift // 3 - 1).astype(F32)
    for n in range(rows):
        o = off[n]
        down = jnp.where(o >= 6, 2, jnp.where(o >= 3, 1, 0))
        centre_right = (o - 3 * down - 1).astype(F32)
        centre_down = (down - 1).astype(F32)
        apart_right = step_right - centre_right
        apart_down = step_down - centre_down
        spv[n : n + 1, :] = -0.5 * (apart_right * apart_right + apart_down * apart_down)
    used = lane < SHIFTS * classes
    espb[x] = jnp.where(used, jnp.exp(spv[...]), 0.0)
    for step, peer in enumerate((right, left, opposite)):
        go(remote(espb.at[x], espb.at[x], s_e.at[step], r_e.at[step], peer, dm))
    class_row = cls[pl.ds(x, 1), :]
    orient_row = ori[pl.ds(x, 1), :]
    prior = jnp.zeros((1, LANES), F32)
    for i in range(classes):
        prior = prior + jnp.where(class_row == i, clp[i], 0.0)
    orient_prior = jnp.zeros((1, LANES), F32)
    for i in range(orients):
        orient_prior = orient_prior + jnp.where(orient_row == i, olp[i], 0.0)
    prior = prior + orient_prior
    column = lax.broadcasted_iota(jnp.int32, (LANES, LANES), 0)
    member = column % classes == class_row
    for t in range(SHIFTS):
        chosen[:, t * LANES : (t + 1) * LANES] = jnp.where(member & (column // classes == t), 1.0, 0.0).astype(BF16)
    width = 2 * coefs // NX
    cols = width // LANES
    spread = LANES // classes
    k = lax.broadcasted_iota(jnp.int32, (spread, width), 1)
    keep[...] = jnp.where(k % cols == lax.broadcasted_iota(jnp.int32, (spread, width), 0), 1.0, 0.0)
    d = lax.broadcasted_iota(jnp.int32, (LANES, width), 0)
    first = ((d // 32) * 32 + (d % 16) * 2 + (d // 16) % 2) * cols
    k = lax.broadcasted_iota(jnp.int32, (LANES, width), 1)
    pick[...] = jnp.where((k >= first) & (k < first + cols), 1.0, 0.0).astype(BF16)
    na[...] = jnp.zeros_like(na)
    s[...] = jnp.zeros_like(s)

    block = SHIFTS * rows

    def turn(to, slot, xs, q):
        def tile(j, carry):
            at_real = pl.ds(pl.multiple_of(j * LANES, LANES), LANES)
            at_imag = pl.ds(pl.multiple_of(ck + j * LANES, LANES), LANES)
            at_table = q * (ck // LANES) + j
            real = pb[xs, q, :, at_real].astype(F32)
            imag = pb[xs, q, :, at_imag].astype(F32)

            def put(t, turned_real, turned_imag):
                at_rows = pl.ds(slot * block + t * rows, rows)
                to[at_rows, at_real] = turned_real.astype(BF16)
                to[at_rows, at_imag] = turned_imag.astype(BF16)

            plain = tw[at_table, 8:9, :]
            put(4, real * plain, imag * plain)
            for i, (plus, minus) in enumerate(PAIRS):
                cosine = tw[at_table, 2 * i : 2 * i + 1, :]
                sine = tw[at_table, 2 * i + 1 : 2 * i + 2, :]
                rc, rs = real * cosine, real * sine
                ic, is_ = imag * cosine, imag * sine
                put(plus, rc - is_, rs + ic)
                put(minus, rc + is_, ic - rs)
            return carry

        for j in range(ck // LANES):
            tile(j, 0)

    def measure(q):
        def tile(j, carry):
            at_real = pl.ds(pl.multiple_of(j * LANES, LANES), LANES)
            at_imag = pl.ds(pl.multiple_of(ck + j * LANES, LANES), LANES)
            weight = w[pl.ds(q * (ck // LANES) + j, 1), :]
            ref_real = rb[q, :, at_real].astype(F32)
            ref_imag = rb[q, :, at_imag].astype(F32)
            na[...] += weight * (ref_real * ref_real + ref_imag * ref_imag)
            return carry

        lax.fori_loop(0, ck // LANES, tile, 0)

    near_rows = 3 * block

    def score_near(q):
        s[0:near_rows, :] += nt(sp[q], rb[q])

    def score_far(q):
        if q == NQ - 1:
            for way in range(2):
                arrived(pb.at[xo, q, :, way * ck : (way + 1) * ck], r_opp.at[q + way])
        else:
            arrived(pb.at[xo, q], r_opp.at[q])
        turn(sp_far, 0, xo, q)
        s[near_rows:, :] += nt(sp_far[...], rb[q])

    def forward_refs(q):
        arrived(rb.at[q, y_rows], r_y.at[q])
        there = rb.at[q, y_rows]
        go(remote(there, there, s_py.at[q], r_py.at[q], partner, dm))

    def refs_ready(q):
        arrived(rb.at[q, p_rows], r_p.at[q])
        arrived(rb.at[q, py_rows], r_py.at[q])

    def other_side(q):
        if q % 2 == 0 and q < NQ - 1:
            arrived(pb.at[xr, q], r_right.at[q])
        elif q % 2 == 1:
            arrived(pb.at[xl, q], r_left.at[q])

    for q in range(NQ):
        turn(sp.at[q], 0, x, q)
    for q in range(NQ):
        forward(q)
        forward_refs(q)
        other_side(q)
        turn(sp.at[q], 1, xl, q)
        turn(sp.at[q], 2, xr, q)
        if q >= NEAR_LAG:
            refs_ready(q - NEAR_LAG)
            score_near(q - NEAR_LAG)
            measure(q - NEAR_LAG)
        if q == 1:
            heard(0)
            tell(1)
        if q == 4:
            heard(1)
            tell(2)
    for q in range(NQ - NEAR_LAG, NQ):
        refs_ready(q)
        score_near(q)
        measure(q)
    for q in range(NQ - HELD):
        score_far(q)
    heard(2)
    tell(3)

    bias = prior - jnp.sum(na[...].T, axis=0, keepdims=True)
    s4 = s.reshape(NX, SHIFTS, rows, LANES)

    def settle(first, last):
        count = (last - first) * rows
        s4[first:last] += bias
        by_shift = [s4[first:last, t].reshape(count, LANES) for t in range(SHIFTS)]
        peak = functools.reduce(jnp.maximum, by_shift)
        peak = jnp.max(peak, axis=1, keepdims=True)
        peak_high, peak_low = split(peak)
        peak = peak_high.astype(F32) + peak_low.astype(F32)
        powers = [jnp.exp(value - peak).astype(BF16) for value in by_shift]
        sums = nt(jnp.concatenate(powers, axis=1), chosen[...])
        tail = jnp.where(lane < LANES - 1, peak_high.astype(F32), peak_low.astype(F32))
        packed = jnp.where(used, sums, tail).astype(BF16)
        for slot in range(first, last):
            xs = (x, xl, xr, xo)[slot]
            place = pl.ds(pl.multiple_of(xs * rows, rows), rows)
            gb[x, place, :] = packed[(slot - first) * rows : (slot - first + 1) * rows]

    settle(0, NX - 1)
    for q in range(NQ - HELD, NQ):
        score_far(q)
    settle(NX - 1, NX)
    parts = NX * rows
    for step, peer in enumerate((right, left, opposite)):
        go(remote(gb.at[x], gb.at[x], s_g.at[step], r_g.at[step], peer, dm))
    for step in range(3):
        src = (x + (NX - 1, 1, 2)[step]) % NX
        arrived(espb.at[src], r_e.at[step])
    for step in range(3):
        src = (x + (NX - 1, 1, 2)[step]) % NX
        arrived(gb.at[src], r_g.at[step])
    for step, (slot, peer) in enumerate(((2, right), (1, left), (3, opposite))):
        go(remote(s4.at[slot], sr.at[x], s_s.at[step], r_s.at[step], peer, dm))
    sr[x] = s4[0]
    blocks = [gb[i].astype(F32) for i in range(NX)]
    peaks = [block[:, LANES - 2 : LANES - 1] + block[:, LANES - 1 : LANES] for block in blocks]
    top = jnp.maximum(jnp.maximum(peaks[0], peaks[1]), jnp.maximum(peaks[2], peaks[3]))
    total = jnp.zeros((parts, LANES), F32)
    for i in range(NX):
        total = total + blocks[i] * jnp.exp(peaks[i] - top)
    total = jnp.where(used, total, 0.0) * espb[...].reshape(parts, LANES)
    norm = jnp.sum(total, axis=1, keepdims=True)
    post = total * (1.0 / norm)
    lz[...] = jnp.broadcast_to(top + jnp.log(norm), (parts, LANES))

    turned = jnp.concatenate([post, jnp.zeros((LANES - parts, LANES), F32)], axis=0).T
    both = jnp.concatenate(split(turned[: SHIFTS * classes, :parts]), axis=0)
    pairs = SHIFTS * classes
    real_side = x < NX // 2
    sign = jnp.where(real_side, -1.0, 1.0).astype(F32) * (1.0 / math.sqrt(npart))
    scale = 1.0 / math.sqrt(npart)
    half = ck // 2
    for piece in range(NQ):
        place = (x % 2) * NQ + piece
        q = place // 2
        within = (place % 2) * half
        at_e = pl.ds(pl.multiple_of(within + jnp.where(real_side, 0, ck), LANES), half)
        at_f = pl.ds(pl.multiple_of(within + jnp.where(real_side, ck, 0), LANES), half)
        e = nn(both, pb[:, q, :, at_e].reshape(parts, half))
        f = nn(both, pb[:, q, :, at_f].reshape(parts, half))
        e = e[:pairs] + e[pairs:]
        f = f[:pairs] + f[pairs:]
        for j in range(half // LANES):
            at_table = place * (half // LANES) + j

            def of(table, t):
                return table[t * classes : (t + 1) * classes, j * LANES : (j + 1) * LANES]

            even = of(e, 4)
            odd = jnp.zeros((classes, LANES), F32)
            for i, (plus, minus) in enumerate(PAIRS):
                cosine = tab[at_table, 2 * i : 2 * i + 1, :]
                sine = tab[at_table, 2 * i + 1 : 2 * i + 2, :]
                even = even + cosine * (of(e, plus) + of(e, minus))
                odd = odd + sine * (of(f, plus) - of(f, minus))
            at_column = piece * half + j * LANES
            cb[:, at_column : at_column + LANES] = scale * even + sign * odd

    laid = jnp.concatenate(
        [
            (jnp.broadcast_to(cb[i : i + 1, :], (spread, width)) * keep[...]).astype(BF16)
            for i in [0, *range(classes - 1, 0, -1)]
        ],
        axis=0,
    )
    wb[...] = nt(pick[...], laid).reshape(NG, NZ, LANES).astype(BF16)
    for step in range(1, NG):
        other = (group + step) % NG
        go(
            remote(
                wb.at[other],
                yb.at[group],
                s_w.at[step],
                r_w.at[group],
                x * NS + other // 2,
                z * 2 + other % 2,
            )
        )
    yb[group] = wb[group]
    for step in range(1, NG):
        src = (group + step) % NG
        arrived(yb.at[src], r_w.at[src])
    heard(3)
    tb[...] = jnp.sum(yb[...].astype(F32), axis=0).reshape(NZ, 1, LANES)
    for step in range(1, NZ):
        other = (z + step) % NZ
        go(remote(tb.at[other], zb.at[z], s_z.at[step], r_z.at[z], me, other * 2 + yh))
    zb[z] = tb[z]

    for step in range(3):
        src = (x + (NX - 1, 1, 2)[step]) % NX
        arrived(sr.at[src], r_s.at[step])
    own_z = lz[pl.ds(pl.multiple_of(x * rows, rows), rows), :]
    for t in range(SHIFTS):
        bias = spv[:, t * classes : t * classes + 1] - own_z
        for i in range(NX):
            post_out[t, :, i * LANES : (i + 1) * LANES] = sr[i, t] + bias

    for copy in sends:
        copy.wait_send()
    for step in range(1, NZ):
        src = (z + step) % NZ
        arrived(zb.at[src], r_z.at[src])
    final = jnp.sum(zb[...], axis=0)
    final = jnp.broadcast_to(final, (classes, LANES))
    final = pltpu.roll(final, 0, 1, stride=spread, stride_axis=0)
    sums_out[...] = final[:, :cols]


def store(post, sums, post_out, sums_out, sems):
    copies = [
        pltpu.make_async_copy(post, post_out, sems.at[0]),
        pltpu.make_async_copy(sums, sums_out, sems.at[1]),
    ]
    for copy in copies:
        copy.start()
    for copy in copies:
        copy.wait()


def solution(mesh):
    assert mesh.shape["ref"] == NX * NS and mesh.shape["dom"] == 2 * NZ

    def local(particles, offsets, references, noise_weight, ref_class, ref_orient, class_logprior, orient_logprior):
        rows, both = particles.shape
        coefs = both // 2
        refs = references.shape[0]
        classes = class_logprior.shape[0]
        orients = orient_logprior.shape[0]
        ck = coefs // NQ
        parts = NX * rows
        width = both // NX
        cols = width // LANES
        npart = rows * NX * NS * 2 * NZ
        assert ck % LANES == 0 and refs * NS == LANES and SHIFTS * classes < LANES - 1 and ck % (2 * LANES) == 0
        dma = pltpu.SemaphoreType.DMA

        def hbm(array):
            return pltpu.with_memory_space_constraint(array, pltpu.HBM)

        log_post, class_sums = pl.pallas_call(
            functools.partial(kernel, coefs, npart, rows, refs, classes, orients),
            out_shape=(
                jax.ShapeDtypeStruct((SHIFTS, rows, NX * LANES), F32),
                jax.ShapeDtypeStruct((classes, cols), F32),
            ),
            in_specs=[pl.BlockSpec(memory_space=pltpu.HBM)] * 9,
            out_specs=(
                pl.BlockSpec(memory_space=pltpu.VMEM),
                pl.BlockSpec(memory_space=pltpu.VMEM),
            ),
            scratch_shapes=[
                pltpu.SMEM((rows,), jnp.int32),
                pltpu.SMEM((classes,), F32),
                pltpu.SMEM((orients,), F32),
                pltpu.VMEM((coefs // LANES, LANES), F32),
                pltpu.VMEM((NX, LANES), jnp.int32),
                pltpu.VMEM((NX, LANES), jnp.int32),
                pltpu.VMEM((coefs // LANES, 8, LANES), F32),
                pltpu.VMEM((coefs // LANES, 16, LANES), F32),
                pltpu.VMEM((NX, NQ, rows, 2 * ck), BF16),
                pltpu.VMEM((NQ, LANES, 2 * ck), BF16),
                pltpu.VMEM((NQ, SHIFTS * 3 * rows, 2 * ck), BF16),
                pltpu.VMEM((SHIFTS * rows, 2 * ck), BF16),
                pltpu.VMEM((SHIFTS * parts, LANES), F32),
                pltpu.VMEM((LANES, LANES), F32),
                pltpu.VMEM((rows, LANES), F32),
                pltpu.VMEM((NX, rows, LANES), F32),
                pltpu.VMEM((NX, parts, LANES), BF16),
                pltpu.VMEM((parts, LANES), F32),
                pltpu.VMEM((LANES, SHIFTS * LANES), BF16),
                pltpu.VMEM((LANES // classes, width), F32),
                pltpu.VMEM((LANES, width), BF16),
                pltpu.VMEM((NX, SHIFTS, rows, LANES), F32),
                pltpu.VMEM((classes, width), F32),
                pltpu.VMEM((NG, NZ, LANES), BF16),
                pltpu.VMEM((NG, NZ, LANES), BF16),
                pltpu.VMEM((NZ, 1, LANES), F32),
                pltpu.VMEM((NZ, 1, LANES), F32),
                pltpu.SemaphoreType.REGULAR((4,)),
                dma((7,)),
            ]
            + [dma((NQ + 1,))] * 14
            + [dma((3,))] * 6
            + [dma((NG,))] * 2
            + [dma((NZ,))] * 2,
            compiler_params=pltpu.CompilerParams(
                collective_id=0, has_side_effects=True, vmem_limit_bytes=32 * 1024 * 1024
            ),
            name="expectation",
        )(
            hbm(offsets),
            hbm(class_logprior),
            hbm(orient_logprior),
            hbm(particles),
            hbm(references),
            hbm(noise_weight.reshape(coefs // LANES, LANES)),
            hbm(ref_class.reshape(NX, LANES)),
            hbm(ref_orient.reshape(NX, LANES)),
            hbm(jnp.asarray(phase_tables(coefs))),
        )
        log_post, class_sums = pl.pallas_call(
            store,
            out_shape=(
                jax.ShapeDtypeStruct(log_post.shape, F32),
                jax.ShapeDtypeStruct(class_sums.shape, F32),
            ),
            in_specs=[pl.BlockSpec(memory_space=pltpu.VMEM)] * 2,
            out_specs=[pl.BlockSpec(memory_space=pltpu.HBM)] * 2,
            scratch_shapes=[dma((2,))],
            compiler_params=pltpu.CompilerParams(vmem_limit_bytes=1024 * 1024),
            name="store",
        )(log_post, class_sums)
        return jnp.swapaxes(log_post, 0, 1), class_sums

    return jax.shard_map(
        local,
        mesh=mesh,
        in_specs=(
            P(("ref", "dom"), None),
            P(("ref", "dom")),
            P("ref", None),
            P(),
            P(),
            P(),
            P(),
            P(),
        ),
        out_specs=(P(("ref", "dom"), None, None), P(None, ("ref", "dom"))),
        check_vma=False,
    )
```

```python
import functools
import math

import jax
import jax.numpy as jnp
import numpy as np
from jax import lax
from jax.experimental import pallas as pl
from jax.experimental.pallas import tpu as pltpu
from jax.sharding import PartitionSpec as P

MESH = pl.DeviceIdType.MESH
SHIFTS = 9
NX = 4
NS = 4
NZ = 16
NG = 8
NQ = 7
NEAR_LAG = 1
HELD = 2
LANES = 128
F32 = jnp.float32
BF16 = jnp.bfloat16
PAIRS = ((5, 3), (7, 1), (8, 0), (6, 2))
STEPS = ((1, 0), (0, 1), (1, 1), (-1, 1))


def phase_tables(count):
    coeffs = np.arange(count)
    fx = (coeffs % 56).astype(np.float32)
    fy = (coeffs // 56 - 32).astype(np.float32)
    rows = []
    for sx, sy in STEPS:
        turning = np.float32(2.0 * math.pi / 96.0) * (np.float32(sx) * fx + np.float32(sy) * fy)
        turning = turning.astype(np.float64)
        rows += [np.cos(turning), np.sin(turning)]
    table = np.stack(rows).astype(np.float32)
    return np.ascontiguousarray(table.reshape(len(rows), -1, LANES).swapaxes(0, 1))


def nt(a, b):
    return lax.dot_general(a, b, (((1,), (1,)), ((), ())), preferred_element_type=F32)


def nn(a, b):
    return lax.dot_general(a, b, (((1,), (0,)), ((), ())), preferred_element_type=F32)


def split(value):
    high = value.astype(BF16)
    return high, (value - high.astype(F32)).astype(BF16)


def kernel(
    coefs,
    npart,
    rows,
    nref,
    classes,
    orients,
    off_hbm,
    clp_hbm,
    olp_hbm,
    part_hbm,
    refs_hbm,
    w_hbm,
    cls_hbm,
    ori_hbm,
    tab_hbm,
    post_out,
    sums_out,
    off,
    clp,
    olp,
    w,
    cls,
    ori,
    tab,
    tw,
    pb,
    rb,
    sp,
    sp_far,
    s,
    na,
    spv,
    espb,
    gb,
    lz,
    chosen,
    keep,
    pick,
    sr,
    cb,
    wb,
    yb,
    tb,
    zb,
    far,
    plane,
    sm,
    lp,
    lr,
    s_right,
    s_left,
    s_fwd,
    r_left,
    r_right,
    r_opp,
    s_y,
    s_p,
    s_py,
    r_y,
    r_p,
    r_py,
    s_e,
    r_e,
    s_g,
    r_g,
    s_s,
    r_s,
    s_w,
    r_w,
    s_z,
    r_z,
):
    ck = coefs // NQ
    me = lax.axis_index("ref")
    dm = lax.axis_index("dom")
    x = me // NS
    sub = me % NS
    yl = sub // 2
    core = sub % 2
    z = dm // 2
    yh = dm % 2
    group = sub * 2 + yh
    right = (me + NS) % (NX * NS)
    left = (me + (NX - 1) * NS) % (NX * NS)
    opposite = (me + 2 * NS) % (NX * NS)
    xl = (x + NX - 1) % NX
    xr = (x + 1) % NX
    xo = (x + 2) % NX
    partner = me + 1 - 2 * core
    y_ref = me + 2 - 4 * yl
    y_dom = dm + core * (1 - 2 * yh)
    refs = nref

    def remote(src, dst, send, recv, ref, dom):
        return pltpu.make_async_remote_copy(
            src_ref=src,
            dst_ref=dst,
            send_sem=send,
            recv_sem=recv,
            device_id=(ref, dom),
            device_id_type=MESH,
        )

    def arrived(buffer, sem):
        pltpu.make_async_copy(buffer, buffer, sem).wait()

    barrier = pltpu.get_barrier_semaphore()

    def beside(distance, act):
        @pl.when(z >= distance)
        def _():
            act(me, dm - 2 * distance)

        @pl.when(z + distance < NZ)
        def _():
            act(me, dm + 2 * distance)

    def near(distance):
        return (z + NZ - distance) // NZ + (2 * NZ - 1 - z - distance) // NZ

    def greet(ref, dom):
        pl.semaphore_signal(barrier, inc=1, device_id=(ref, dom), device_id_type=MESH)

    y = yh * 2 + yl
    neighbours = [(right, dm), (left, dm), (partner, dm)]
    for turned in (1, 3):
        other_y = (y + turned) % 4
        for swap in range(2):
            other_core = (core + swap) % 2
            neighbours.append((x * NS + (other_y % 2) * 2 + other_core, z * 2 + other_y // 2))
    for ref, dom in neighbours:
        greet(ref, dom)
    beside(1, greet)
    smalls = (
        (off_hbm, off),
        (clp_hbm, clp),
        (olp_hbm, olp),
        (w_hbm, w),
        (cls_hbm, cls),
        (ori_hbm, ori),
        (tab_hbm, tab),
    )
    own_rows = pl.ds(pl.multiple_of(sub * refs, refs), refs)
    for q in range(NQ):
        for half in range(2):
            pltpu.make_async_copy(
                part_hbm.at[:, pl.ds(half * coefs + q * ck, ck)],
                pb.at[x, q, :, pl.ds(half * ck, ck)],
                lp.at[q],
            ).start()
            pltpu.make_async_copy(
                refs_hbm.at[:, pl.ds(half * coefs + q * ck, ck)],
                rb.at[q, own_rows, pl.ds(half * ck, ck)],
                lr.at[q],
            ).start()
    for i, (src, dst) in enumerate(smalls):
        pltpu.make_async_copy(src, dst, sm.at[i]).start()
    pl.semaphore_wait(barrier, len(neighbours) + near(1))

    for ref, dom in neighbours:
        pl.semaphore_signal(plane, inc=1, device_id=(ref, dom), device_id_type=MESH)

    def tell(i):
        def one(ref, dom):
            pl.semaphore_signal(far.at[i], inc=1, device_id=(ref, dom), device_id_type=MESH)

        beside(2**i, one)

    def heard(i):
        pl.semaphore_wait(far.at[i], near(2**i))

    tell(0)

    sends = []

    def go(copy):
        copy.start()
        sends.append(copy)

    def send_own(q):
        go(remote(pb.at[x, q], pb.at[x, q], s_right.at[q], r_left.at[q], right, dm))
        go(remote(pb.at[x, q], pb.at[x, q], s_left.at[q], r_right.at[q], left, dm))

    def forward(q):
        if q % 2 == 0 or q == NQ - 1:
            arrived(pb.at[xl, q], r_left.at[q])
        if q % 2 == 1 or q == NQ - 1:
            arrived(pb.at[xr, q], r_right.at[q])
        if q == NQ - 1:
            for way, (xs, peer) in enumerate(((xl, right), (xr, left))):
                piece = pb.at[xs, q, :, way * ck : (way + 1) * ck]
                go(remote(piece, piece, s_fwd.at[q + way], r_opp.at[q + way], peer, dm))
        elif q % 2 == 0:
            go(remote(pb.at[xl, q], pb.at[xl, q], s_fwd.at[q], r_opp.at[q], right, dm))
        else:
            go(remote(pb.at[xr, q], pb.at[xr, q], s_fwd.at[q], r_opp.at[q], left, dm))

    y_rows = pl.ds(pl.multiple_of((y_ref % NS) * refs, refs), refs)
    p_rows = pl.ds(pl.multiple_of((partner % NS) * refs, refs), refs)
    py_sub = (partner % NS) + 2 - 4 * yl
    py_rows = pl.ds(pl.multiple_of(py_sub * refs, refs), refs)

    for q in range(NQ):
        arrived(pb.at[x, q], lp.at[q])
        send_own(q)
        arrived(rb.at[q, own_rows], lr.at[q])
        own = rb.at[q, own_rows]
        go(remote(own, own, s_y.at[q], r_y.at[q], y_ref, y_dom))
        go(remote(own, own, s_p.at[q], r_p.at[q], partner, dm))

    for i, (src, dst) in enumerate(smalls):
        pltpu.make_async_copy(src, dst, sm.at[i]).wait()
    for i in range(coefs // LANES):
        two_w = 2.0 * w[i : i + 1, :]
        tw[i, 0:8, :] = tab[i] * two_w
        tw[i, 8:9, :] = two_w
    lane = lax.broadcasted_iota(jnp.int32, (1, LANES), 1)
    shift = lane // classes
    step_right = (shift % 3 - 1).astype(F32)
    step_down = (shift // 3 - 1).astype(F32)
    for n in range(rows):
        o = off[n]
        down = jnp.where(o >= 6, 2, jnp.where(o >= 3, 1, 0))
        centre_right = (o - 3 * down - 1).astype(F32)
        centre_down = (down - 1).astype(F32)
        apart_right = step_right - centre_right
        apart_down = step_down - centre_down
        spv[n : n + 1, :] = -0.5 * (apart_right * apart_right + apart_down * apart_down)
    used = lane < SHIFTS * classes
    espb[x] = jnp.where(used, jnp.exp(spv[...]), 0.0)
    class_row = cls[pl.ds(x, 1), :]
    orient_row = ori[pl.ds(x, 1), :]
    prior = jnp.zeros((1, LANES), F32)
    for i in range(classes):
        prior = prior + jnp.where(class_row == i, clp[i], 0.0)
    orient_prior = jnp.zeros((1, LANES), F32)
    for i in range(orients):
        orient_prior = orient_prior + jnp.where(orient_row == i, olp[i], 0.0)
    prior = prior + orient_prior
    column = lax.broadcasted_iota(jnp.int32, (LANES, LANES), 0)
    member = column % classes == class_row
    for t in range(SHIFTS):
        chosen[:, t * LANES : (t + 1) * LANES] = jnp.where(member & (column // classes == t), 1.0, 0.0).astype(BF16)
    width = 2 * coefs // NX
    cols = width // LANES
    spread = LANES // classes
    k = lax.broadcasted_iota(jnp.int32, (spread, width), 1)
    keep[...] = jnp.where(k % cols == lax.broadcasted_iota(jnp.int32, (spread, width), 0), 1.0, 0.0)
    d = lax.broadcasted_iota(jnp.int32, (LANES, width), 0)
    first = ((d // 32) * 32 + (d % 16) * 2 + (d // 16) % 2) * cols
    k = lax.broadcasted_iota(jnp.int32, (LANES, width), 1)
    pick[...] = jnp.where((k >= first) & (k < first + cols), 1.0, 0.0).astype(BF16)
    na[...] = jnp.zeros_like(na)
    s[...] = jnp.zeros_like(s)

    block = SHIFTS * rows

    def turn(to, slot, xs, q):
        def tile(j, carry):
            at_real = pl.ds(pl.multiple_of(j * LANES, LANES), LANES)
            at_imag = pl.ds(pl.multiple_of(ck + j * LANES, LANES), LANES)
            at_table = q * (ck // LANES) + j
            real = pb[xs, q, :, at_real].astype(F32)
            imag = pb[xs, q, :, at_imag].astype(F32)

            def put(t, turned_real, turned_imag):
                at_rows = pl.ds(slot * block + t * rows, rows)
                to[at_rows, at_real] = turned_real.astype(BF16)
                to[at_rows, at_imag] = turned_imag.astype(BF16)

            plain = tw[at_table, 8:9, :]
            put(4, real * plain, imag * plain)
            for i, (plus, minus) in enumerate(PAIRS):
                cosine = tw[at_table, 2 * i : 2 * i + 1, :]
                sine = tw[at_table, 2 * i + 1 : 2 * i + 2, :]
                rc, rs = real * cosine, real * sine
                ic, is_ = imag * cosine, imag * sine
                put(plus, rc - is_, rs + ic)
                put(minus, rc + is_, ic - rs)
            return carry

        for j in range(ck // LANES):
            tile(j, 0)

    def measure(q):
        def tile(j, carry):
            at_real = pl.ds(pl.multiple_of(j * LANES, LANES), LANES)
            at_imag = pl.ds(pl.multiple_of(ck + j * LANES, LANES), LANES)
            weight = w[pl.ds(q * (ck // LANES) + j, 1), :]
            ref_real = rb[q, :, at_real].astype(F32)
            ref_imag = rb[q, :, at_imag].astype(F32)
            na[...] += weight * (ref_real * ref_real + ref_imag * ref_imag)
            return carry

        lax.fori_loop(0, ck // LANES, tile, 0)

    near_rows = 3 * block

    def score_near(q):
        s[0:near_rows, :] += nt(sp[q], rb[q])

    def score_far(q):
        if q == NQ - 1:
            for way in range(2):
                arrived(pb.at[xo, q, :, way * ck : (way + 1) * ck], r_opp.at[q + way])
        else:
            arrived(pb.at[xo, q], r_opp.at[q])
        turn(sp_far, 0, xo, q)
        s[near_rows:, :] += nt(sp_far[...], rb[q])

    def forward_refs(q):
        arrived(rb.at[q, y_rows], r_y.at[q])
        there = rb.at[q, y_rows]
        go(remote(there, there, s_py.at[q], r_py.at[q], partner, dm))

    def refs_ready(q):
        arrived(rb.at[q, p_rows], r_p.at[q])
        arrived(rb.at[q, py_rows], r_py.at[q])

    def other_side(q):
        if q % 2 == 0 and q < NQ - 1:
            arrived(pb.at[xr, q], r_right.at[q])
        elif q % 2 == 1 and q < NQ - 1:
            arrived(pb.at[xl, q], r_left.at[q])

    for q in range(NQ):
        turn(sp.at[q], 0, x, q)
    for q in range(NQ):
        forward(q)
        forward_refs(q)
        other_side(q)
        turn(sp.at[q], 1, xl, q)
        turn(sp.at[q], 2, xr, q)
        if q >= NEAR_LAG:
            refs_ready(q - NEAR_LAG)
            score_near(q - NEAR_LAG)
            measure(q - NEAR_LAG)
        if q == 1:
            pl.semaphore_wait(plane, len(neighbours))
            for step, peer in enumerate((right, left, opposite)):
                go(remote(espb.at[x], espb.at[x], s_e.at[step], r_e.at[step], peer, dm))
            heard(0)
            tell(1)
        if q == 4:
            heard(1)
            tell(2)
    for q in range(NQ - NEAR_LAG, NQ):
        refs_ready(q)
        score_near(q)
        measure(q)
    for q in range(NQ - HELD):
        score_far(q)
    heard(2)
    tell(3)

    bias = prior - jnp.sum(na[...].T, axis=0, keepdims=True)
    s4 = s.reshape(NX, SHIFTS, rows, LANES)

    def settle(first, last):
        count = (last - first) * rows
        s4[first:last] += bias
        by_shift = [s4[first:last, t].reshape(count, LANES) for t in range(SHIFTS)]
        peak = functools.reduce(jnp.maximum, by_shift)
        peak = jnp.max(peak, axis=1, keepdims=True)
        peak_high, peak_low = split(peak)
        peak = peak_high.astype(F32) + peak_low.astype(F32)
        powers = [jnp.exp(value - peak).astype(BF16) for value in by_shift]
        sums = nt(jnp.concatenate(powers, axis=1), chosen[...])
        tail = jnp.where(lane < LANES - 1, peak_high.astype(F32), peak_low.astype(F32))
        packed = jnp.where(used, sums, tail).astype(BF16)
        for slot in range(first, last):
            xs = (x, xl, xr, xo)[slot]
            place = pl.ds(pl.multiple_of(xs * rows, rows), rows)
            gb[x, place, :] = packed[(slot - first) * rows : (slot - first + 1) * rows]

    settle(0, NX - 1)
    for q in range(NQ - HELD, NQ):
        score_far(q)
    settle(NX - 1, NX)
    parts = NX * rows
    for step, peer in enumerate((right, left, opposite)):
        go(remote(gb.at[x], gb.at[x], s_g.at[step], r_g.at[step], peer, dm))
    for step in range(3):
        src = (x + (NX - 1, 1, 2)[step]) % NX
        arrived(espb.at[src], r_e.at[step])
    for step in range(3):
        src = (x + (NX - 1, 1, 2)[step]) % NX
        arrived(gb.at[src], r_g.at[step])
    for step, (slot, peer) in enumerate(((2, right), (1, left), (3, opposite))):
        go(remote(s4.at[slot], sr.at[x], s_s.at[step], r_s.at[step], peer, dm))
    sr[x] = s4[0]
    blocks = [gb[i].astype(F32) for i in range(NX)]
    peaks = [block[:, LANES - 2 : LANES - 1] + block[:, LANES - 1 : LANES] for block in blocks]
    top = jnp.maximum(jnp.maximum(peaks[0], peaks[1]), jnp.maximum(peaks[2], peaks[3]))
    total = jnp.zeros((parts, LANES), F32)
    for i in range(NX):
        total = total + blocks[i] * jnp.exp(peaks[i] - top)
    total = jnp.where(used, total, 0.0) * espb[...].reshape(parts, LANES)
    norm = jnp.sum(total, axis=1, keepdims=True)
    post = total * (1.0 / norm)
    lz[...] = jnp.broadcast_to(top + jnp.log(norm), (parts, LANES))

    turned = jnp.concatenate([post, jnp.zeros((LANES - parts, LANES), F32)], axis=0).T
    both = jnp.concatenate(split(turned[: SHIFTS * classes, :parts]), axis=0)
    pairs = SHIFTS * classes
    real_side = x < NX // 2
    sign = jnp.where(real_side, -1.0, 1.0).astype(F32) * (1.0 / math.sqrt(npart))
    scale = 1.0 / math.sqrt(npart)
    half = ck // 2
    for piece in range(NQ):
        place = (x % 2) * NQ + piece
        q = place // 2
        within = (place % 2) * half
        at_e = pl.ds(pl.multiple_of(within + jnp.where(real_side, 0, ck), LANES), half)
        at_f = pl.ds(pl.multiple_of(within + jnp.where(real_side, ck, 0), LANES), half)
        e = nn(both, pb[:, q, :, at_e].reshape(parts, half))
        f = nn(both, pb[:, q, :, at_f].reshape(parts, half))
        e = e[:pairs] + e[pairs:]
        f = f[:pairs] + f[pairs:]
        for j in range(half // LANES):
            at_table = place * (half // LANES) + j

            def of(table, t):
                return table[t * classes : (t + 1) * classes, j * LANES : (j + 1) * LANES]

            even = of(e, 4)
            odd = jnp.zeros((classes, LANES), F32)
            for i, (plus, minus) in enumerate(PAIRS):
                cosine = tab[at_table, 2 * i : 2 * i + 1, :]
                sine = tab[at_table, 2 * i + 1 : 2 * i + 2, :]
                even = even + cosine * (of(e, plus) + of(e, minus))
                odd = odd + sine * (of(f, plus) - of(f, minus))
            at_column = piece * half + j * LANES
            cb[:, at_column : at_column + LANES] = scale * even + sign * odd

    laid = jnp.concatenate(
        [
            (jnp.broadcast_to(cb[i : i + 1, :], (spread, width)) * keep[...]).astype(BF16)
            for i in [0, *range(classes - 1, 0, -1)]
        ],
        axis=0,
    )
    wb[...] = nt(pick[...], laid).reshape(NG, NZ, LANES).astype(BF16)
    for step in range(1, NG):
        other = (group + step) % NG
        go(
            remote(
                wb.at[other],
                yb.at[group],
                s_w.at[step],
                r_w.at[group],
                x * NS + other // 2,
                z * 2 + other % 2,
            )
        )
    yb[group] = wb[group]
    for step in range(1, NG):
        src = (group + step) % NG
        arrived(yb.at[src], r_w.at[src])
    heard(3)
    tb[...] = jnp.sum(yb[...].astype(F32), axis=0).reshape(NZ, 1, LANES)
    for step in range(1, NZ):
        other = (z + step) % NZ
        go(remote(tb.at[other], zb.at[z], s_z.at[step], r_z.at[z], me, other * 2 + yh))
    zb[z] = tb[z]

    for step in range(3):
        src = (x + (NX - 1, 1, 2)[step]) % NX
        arrived(sr.at[src], r_s.at[step])
    own_z = lz[pl.ds(pl.multiple_of(x * rows, rows), rows), :]
    for t in range(SHIFTS):
        bias = spv[:, t * classes : t * classes + 1] - own_z
        for i in range(NX):
            post_out[t, :, i * LANES : (i + 1) * LANES] = sr[i, t] + bias

    for copy in sends:
        copy.wait_send()
    for step in range(1, NZ):
        src = (z + step) % NZ
        arrived(zb.at[src], r_z.at[src])
    final = jnp.sum(zb[...], axis=0)
    final = jnp.broadcast_to(final, (classes, LANES))
    final = pltpu.roll(final, 0, 1, stride=spread, stride_axis=0)
    sums_out[...] = final[:, :cols]


def store(post, sums, post_out, sums_out, sems):
    copies = [
        pltpu.make_async_copy(post, post_out, sems.at[0]),
        pltpu.make_async_copy(sums, sums_out, sems.at[1]),
    ]
    for copy in copies:
        copy.start()
    for copy in copies:
        copy.wait()


def solution(mesh):
    assert mesh.shape["ref"] == NX * NS and mesh.shape["dom"] == 2 * NZ

    def local(particles, offsets, references, noise_weight, ref_class, ref_orient, class_logprior, orient_logprior):
        rows, both = particles.shape
        coefs = both // 2
        refs = references.shape[0]
        classes = class_logprior.shape[0]
        orients = orient_logprior.shape[0]
        ck = coefs // NQ
        parts = NX * rows
        width = both // NX
        cols = width // LANES
        npart = rows * NX * NS * 2 * NZ
        assert ck % LANES == 0 and refs * NS == LANES and SHIFTS * classes < LANES - 1 and ck % (2 * LANES) == 0
        dma = pltpu.SemaphoreType.DMA

        def hbm(array):
            return pltpu.with_memory_space_constraint(array, pltpu.HBM)

        log_post, class_sums = pl.pallas_call(
            functools.partial(kernel, coefs, npart, rows, refs, classes, orients),
            out_shape=(
                jax.ShapeDtypeStruct((SHIFTS, rows, NX * LANES), F32),
                jax.ShapeDtypeStruct((classes, cols), F32),
            ),
            in_specs=[pl.BlockSpec(memory_space=pltpu.HBM)] * 9,
            out_specs=(
                pl.BlockSpec(memory_space=pltpu.VMEM),
                pl.BlockSpec(memory_space=pltpu.VMEM),
            ),
            scratch_shapes=[
                pltpu.SMEM((rows,), jnp.int32),
                pltpu.SMEM((classes,), F32),
                pltpu.SMEM((orients,), F32),
                pltpu.VMEM((coefs // LANES, LANES), F32),
                pltpu.VMEM((NX, LANES), jnp.int32),
                pltpu.VMEM((NX, LANES), jnp.int32),
                pltpu.VMEM((coefs // LANES, 8, LANES), F32),
                pltpu.VMEM((coefs // LANES, 16, LANES), F32),
                pltpu.VMEM((NX, NQ, rows, 2 * ck), BF16),
                pltpu.VMEM((NQ, LANES, 2 * ck), BF16),
                pltpu.VMEM((NQ, SHIFTS * 3 * rows, 2 * ck), BF16),
                pltpu.VMEM((SHIFTS * rows, 2 * ck), BF16),
                pltpu.VMEM((SHIFTS * parts, LANES), F32),
                pltpu.VMEM((LANES, LANES), F32),
                pltpu.VMEM((rows, LANES), F32),
                pltpu.VMEM((NX, rows, LANES), F32),
                pltpu.VMEM((NX, parts, LANES), BF16),
                pltpu.VMEM((parts, LANES), F32),
                pltpu.VMEM((LANES, SHIFTS * LANES), BF16),
                pltpu.VMEM((LANES // classes, width), F32),
                pltpu.VMEM((LANES, width), BF16),
                pltpu.VMEM((NX, SHIFTS, rows, LANES), F32),
                pltpu.VMEM((classes, width), F32),
                pltpu.VMEM((NG, NZ, LANES), BF16),
                pltpu.VMEM((NG, NZ, LANES), BF16),
                pltpu.VMEM((NZ, 1, LANES), F32),
                pltpu.VMEM((NZ, 1, LANES), F32),
                pltpu.SemaphoreType.REGULAR((4,)),
                pltpu.SemaphoreType.REGULAR,
                dma((7,)),
            ]
            + [dma((NQ + 1,))] * 14
            + [dma((3,))] * 6
            + [dma((NG,))] * 2
            + [dma((NZ,))] * 2,
            compiler_params=pltpu.CompilerParams(
                collective_id=0, has_side_effects=True, vmem_limit_bytes=32 * 1024 * 1024
            ),
            name="expectation",
        )(
            hbm(offsets),
            hbm(class_logprior),
            hbm(orient_logprior),
            hbm(particles),
            hbm(references),
            hbm(noise_weight.reshape(coefs // LANES, LANES)),
            hbm(ref_class.reshape(NX, LANES)),
            hbm(ref_orient.reshape(NX, LANES)),
            hbm(jnp.asarray(phase_tables(coefs))),
        )
        log_post, class_sums = pl.pallas_call(
            store,
            out_shape=(
                jax.ShapeDtypeStruct(log_post.shape, F32),
                jax.ShapeDtypeStruct(class_sums.shape, F32),
            ),
            in_specs=[pl.BlockSpec(memory_space=pltpu.VMEM)] * 2,
            out_specs=[pl.BlockSpec(memory_space=pltpu.HBM)] * 2,
            scratch_shapes=[dma((2,))],
            compiler_params=pltpu.CompilerParams(vmem_limit_bytes=1024 * 1024),
            name="store",
        )(log_post, class_sums)
        return jnp.swapaxes(log_post, 0, 1), class_sums

    return jax.shard_map(
        local,
        mesh=mesh,
        in_specs=(
            P(("ref", "dom"), None),
            P(("ref", "dom")),
            P("ref", None),
            P(),
            P(),
            P(),
            P(),
            P(),
        ),
        out_specs=(P(("ref", "dom"), None, None), P(None, ("ref", "dom"))),
        check_vma=False,
    )
```
